16 devices in a mesh: rep: 2 (over y, z), dp: 8 (over x, core).
Axes of the slice: x: 4, y: 2, z: 1, core: 2. Of those that a mesh axis runs over, the one named last changes fastest.
The devices are a block of a 4x4x8 slice.
Arguments:
- x: bfloat16 [16, 2048, 896], P(('rep', 'dp')), parts along dimension 0
- dy: bfloat16 [16, 2048, 896], P(('rep', 'dp')), parts along dimension 0
- w_gate: bfloat16 [2, 896, 2560], replicated
- w_up: bfloat16 [2, 896, 2560], replicated
- w_down: bfloat16 [2, 2560, 896], replicated
- m_w_gate: float32 [2, 896, 2560], P(None, 'dp')
- m_w_up: float32 [2, 896, 2560], P(None, 'dp')
- m_w_down: float32 [2, 2560, 896], P(None, 'dp')
- v_w_gate: float32 [2, 896, 2560], P(None, 'dp')
- v_w_up: float32 [2, 896, 2560], P(None, 'dp')
- v_w_down: float32 [2, 2560, 896], P(None, 'dp')
Outputs:
- output 1: bfloat16 [4, 896, 2560], P('rep'), parts along dimension 0
- output 2: bfloat16 [4, 896, 2560], P('rep'), parts along dimension 0
- output 3: bfloat16 [4, 2560, 896], P('rep'), parts along dimension 0
- output 4: float32 [4, 896, 2560], P('rep', 'dp'), parts along dimension 0
- output 5: float32 [4, 896, 2560], P('rep', 'dp'), parts along dimension 0
- output 6: float32 [4, 2560, 896], P('rep', 'dp'), parts along dimension 0
- output 7: float32 [4, 896, 2560], P('rep', 'dp'), parts along dimension 0
- output 8: float32 [4, 896, 2560], P('rep', 'dp'), parts along dimension 0
- output 9: float32 [4, 2560, 896], P('rep', 'dp'), parts along dimension 0
There are 2 independent parts. The reference program is written for one: setup_inputs(seed, part) draws one part's arguments, and reference() takes and returns one part's arrays. A program takes and returns all parts, laid end to end along the dimension named above; an argument that names none is the same for every part.
All inputs are finite; a program needn't handle non-finite values.
Results may differ from the reference program's by a relative error of at most 0.022.
Values are sent between devices in bfloat16 or wider.
A program may use at most 768 MiB of HBM per device.

```python
import jax
import jax.numpy as jnp
from jax import lax

SEQUENCES = 8
TOKENS = 2048
D = 896
FF = 2560
LAYERS = 2
NAMES = ("w_gate", "w_up", "w_down")
SHAPES = {"w_gate": (LAYERS, D, FF), "w_up": (LAYERS, D, FF), "w_down": (LAYERS, FF, D)}


def bump(key, n, height):
    away = (jnp.arange(n, dtype=jnp.int32) - jax.random.randint(key, (), 0, n, jnp.int32)) % n
    return jnp.where(away < n // 8, height, 1.0)


def together(key, own, strength):
    shared = jax.random.normal(key, own.shape[1:], jnp.float32)
    return (own + strength * shared) * lax.rsqrt(1 + strength * strength)


def setup_inputs(seed: int = 0, part: int = 0) -> dict:
    kx, kdy, ka, kb, kz, kf, kh, kl, *keys = jax.random.split(jax.random.key(seed), 8 + 3 * len(NAMES))
    kx, kdy, ka, kb = (jax.random.fold_in(k, part) for k in (kx, kdy, ka, kb))
    kw, km, kv = (keys[i::3] for i in range(3))
    shape = (SEQUENCES, TOKENS, D)
    much_x, much_dy = jax.random.uniform(kz, (2,), jnp.float32, 0.0, 1.0)
    loud = 2.0 ** jax.random.uniform(jax.random.fold_in(kz, 1), (), jnp.float32, -1.0, 2.0)
    layers = 2.0 ** jax.random.uniform(kl, (LAYERS, 1, 1), jnp.float32, -1.0, 1.0)
    x = together(ka, jax.random.normal(kx, shape, jnp.float32), much_x) * bump(kf, D, 4.0)
    dy = together(kb, jax.random.normal(kdy, shape, jnp.float32), much_dy)
    drawn = {"x": x.astype(jnp.bfloat16), "dy": (loud * dy * (SEQUENCES * TOKENS) ** -0.5).astype(jnp.bfloat16)}
    for key, name in zip(kw, NAMES, strict=True):
        w = jax.random.normal(key, SHAPES[name], jnp.float32) * SHAPES[name][1] ** -0.5
        drawn[name] = (w * {"w_gate": 1.0, "w_up": bump(kh, FF, 4.0), "w_down": layers}[name]).astype(jnp.bfloat16)
    for key, name in zip(km, NAMES, strict=True):
        drawn[f"m_{name}"] = 0.1 * jax.random.normal(key, SHAPES[name], jnp.float32)
    for key, name in zip(kv, NAMES, strict=True):
        drawn[f"v_{name}"] = jax.random.uniform(key, SHAPES[name], jnp.float32, 0.005, 0.015)
    return drawn


def matmul(a, w):
    return jnp.dot(a, w, preferred_element_type=jnp.float32).astype(jnp.bfloat16)


def normed(h):
    wide = h.astype(jnp.float32)
    scale = lax.rsqrt(jnp.mean(wide**2, -1, keepdims=True) + 1e-6)
    return (wide * scale).astype(jnp.bfloat16)


def layer(h, w):
    a = normed(h)
    gate = jnp.dot(a, w["w_gate"], preferred_element_type=jnp.float32)
    up = jnp.dot(a, w["w_up"], preferred_element_type=jnp.float32)
    return h + matmul((jax.nn.silu(gate) * up).astype(jnp.bfloat16), w["w_down"])


def adamw(w, m, v, g):
    m = 0.9 * m + 0.1 * g
    v = 0.95 * v + 0.05 * g * g
    step = m * lax.rsqrt(v + 1e-8) + 0.1 * w
    return (w - 0.02 * step).astype(jnp.bfloat16), m, v


def clipped(gradients, sum_of_squares, count):
    factor = jnp.minimum(1.0, 0.5 * lax.rsqrt(sum_of_squares / count + 1e-30))
    return [g * factor for g in gradients]


def stack(weights, h):
    return lax.scan(lambda h, w: (layer(h, w), None), h, weights)[0]


def reference(x, dy, w_gate, w_up, w_down, m_w_gate, m_w_up, m_w_down, v_w_gate, v_w_up, v_w_down):
    weights = dict(zip(NAMES, (w_gate, w_up, w_down), strict=True))

    def take(so_far, sequence):
        h, by_y = sequence
        _, back = jax.vjp(lambda w: stack(w, h), weights)
        return jax.tree.map(lambda total, term: total + term.astype(jnp.float32), so_far, back(by_y)[0]), None

    none_yet = {name: jnp.zeros(w.shape, jnp.float32) for name, w in weights.items()}
    by_weights, _ = lax.scan(take, none_yet, (x, dy))
    gradients = [by_weights[name].astype(jnp.bfloat16).astype(jnp.float32) for name in NAMES]
    gradients = clipped(gradients, sum(jnp.sum(g * g) for g in gradients), sum(g.size for g in gradients))
    new = [
        adamw(w.astype(jnp.float32), m, v, g)
        for w, m, v, g in zip((w_gate, w_up, w_down), (m_w_gate, m_w_up, m_w_down), (v_w_gate, v_w_up, v_w_down), gradients, strict=True)
    ]
    return tuple(one[which] for which in range(3) for one in new)
```

```python
import functools

import jax
import jax.numpy as jnp
from jax import lax
from jax.experimental import pallas as pl
from jax.experimental.pallas import tpu as pltpu
from jax.sharding import PartitionSpec as P

F32, BF16 = jnp.float32, jnp.bfloat16
VMEM_LIMIT = 63 * 1024 * 1024
NT = (((1,), (1,)), ((), ()))
TILE = 512
ROWS = 256


def dot(a, b, dims=(((1,), (0,)), ((), ()))):
    return lax.dot_general(a, b, dims, preferred_element_type=F32)


def scale_of(wide):
    return lax.rsqrt(jnp.mean(wide * wide, -1, keepdims=True) + 1e-6)


def normed(h):
    wide = h.astype(F32)
    return (wide * scale_of(wide)).astype(BF16)


def chunks(total, size):
    return [slice(at, min(at + size, total)) for at in range(0, total, size)]


def gated(gate, up, dact):
    s = jax.nn.sigmoid(gate)
    silu = gate * s
    return (dact * up * (s + silu * (1 - s))).astype(BF16), (dact * silu).astype(BF16)


def rows_kernel(x, dy, wg0, wu0, wd0, wg1, wu1, wd1, b, at, gate0, up0):
    cols = chunks(wg0.shape[1], 512)
    a = normed(x[...])
    at[3] = a.T
    for c in cols:
        gate, up = dot(a, wg0[:, c]), dot(a, wu0[:, c])
        gate0[:, c], up0[:, c] = gate, up
        b[3, :, c] = (jax.nn.silu(gate) * up).astype(BF16)
    h = x[...] + dot(b[3], wd0[...]).astype(BF16)
    a = normed(h)
    at[1] = a.T
    d = dy[...]
    at[0] = d.T
    for c in cols:
        gate, up = dot(a, wg1[:, c]), dot(a, wu1[:, c])
        dact = dot(d, wd1[c, :], NT).astype(BF16).astype(F32)
        b[0, :, c] = (jax.nn.silu(gate) * up).astype(BF16)
        b[1, :, c], b[2, :, c] = gated(gate, up, dact)
    da = dot(b[1], wg1[...], NT).astype(BF16) + dot(b[2], wu1[...], NT).astype(BF16)
    da, wide = da.astype(F32), h.astype(F32)
    scale = scale_of(wide)
    inner = jnp.mean(da * wide, -1, keepdims=True)
    d = d + (da * scale - wide * (scale * scale * scale * inner)).astype(BF16)
    at[2] = d.T
    for c in cols:
        dact = dot(d, wd0[c, :], NT).astype(BF16).astype(F32)
        b[4, :, c], b[5, :, c] = gated(gate0[:, c], up0[:, c], dact)


def row_local(x, dy, wg, wu, wd):
    t, d = x.shape
    f = wg.shape[2]
    resident = lambda w, n: pl.BlockSpec((pl.squeezed, *w.shape[1:]), lambda i: (n, 0, 0), pipeline_mode=pl.Buffered(1))
    rows = pl.BlockSpec((ROWS, d), lambda i: (i, 0))
    return pl.pallas_call(
        rows_kernel,
        grid=(t // ROWS,),
        in_specs=[rows, rows] + [resident(w, n) for n in (0, 1) for w in (wg, wu, wd)],
        out_specs=[pl.BlockSpec((6, ROWS, f), lambda i: (0, i, 0)), pl.BlockSpec((4, d, ROWS), lambda i: (0, 0, i))],
        out_shape=[jax.ShapeDtypeStruct((6, t, f), BF16), jax.ShapeDtypeStruct((4, d, t), BF16)],
        scratch_shapes=[pltpu.VMEM((ROWS, f), F32), pltpu.VMEM((ROWS, f), F32)],
        compiler_params=pltpu.CompilerParams(vmem_limit_bytes=VMEM_LIMIT),
        cost_estimate=pl.CostEstimate(flops=18 * t * d * f, bytes_accessed=150 * 2**20, transcendentals=0),
        name="rows",
    )(x, dy, wg, wu, wd, wg, wu, wd)


class Place:
    def __init__(self, devices):
        assert devices == 8
        self.devices = devices
        self.me = lax.axis_index("dp")
        self.chip, self.core = self.me // 2, self.me % 2

    def block(self, step):
        return (self.chip + step) % 4 * 2 + self.core

    def sibling_block(self, step):
        return (self.chip + step) % 4 * 2 + 1 - self.core

    def barrier(self, peers):
        semaphore = pltpu.get_barrier_semaphore()
        for peer in peers:
            pl.semaphore_signal(semaphore, inc=1, device_id={"dp": peer}, device_id_type=pl.DeviceIdType.MESH)
        pl.semaphore_wait(semaphore, len(peers))


def send(src, dst, sems, at, to):
    return pltpu.make_async_remote_copy(
        src_ref=src, dst_ref=dst, send_sem=sems[0].at[at], recv_sem=sems[1].at[at], device_id={"dp": to}, device_id_type=pl.DeviceIdType.MESH
    )


def each_row(count, body, size=16):
    lax.fori_loop(0, count // size, lambda i, c: body(pl.ds(pl.multiple_of(i * size, size), size), c) or c, 0)


def grads_kernel(
    devices, at, b, out_wide, out_tall, out_total, wide, tall, sib_wide, sib_tall, transit_wide, transit_tall, end_wide, end_tall, part, totals, sends, recvs
):
    step = pl.program_id(0)
    per = b.shape[1] and wide.shape[2] // TILE
    which, tile = step // per, step % per
    place = Place(devices)
    me = place.me
    peers = [(me + j) % devices for j in range(1, devices)]
    sibling = place.sibling_block(0)
    sems = (sends, recvs)
    low, high = wide.shape[1] // devices, tall.shape[0] // devices

    @pl.when(step == 0)
    def _():
        part[...] = jnp.zeros_like(part)
        place.barrier(peers)

    class Sum:
        def __init__(self, k):
            self.k, self.is_tall = k, k % 3 == 0
            n = k // 3
            if self.is_tall:
                self.rows, self.mine, self.sib = high, tall, sib_tall
                self.transit, self.end, self.out = [transit_tall.at[n, i] for i in (0, 1)], [end_tall.at[n, i] for i in (0, 1)], out_tall.at[n]
                self.halves = [(pl.ds(i * high // 2, high // 2), slice(None)) for i in (0, 1)]
            else:
                slot = k % 3 - 1
                self.rows, self.mine, self.sib = low, wide.at[slot], sib_wide.at[slot]
                at = 2 * n + slot
                self.transit, self.end, self.out = [transit_wide.at[at, i] for i in (0, 1)], [end_wide.at[at, i] for i in (0, 1)], out_wide.at[at]
                c = wide.shape[2] // 2
                self.halves = [(slice(None), slice(i * c, (i + 1) * c)) for i in (0, 1)]

        def block(self, number):
            return self.mine.at[pl.ds(pl.multiple_of(number * self.rows, 16), self.rows), :]

        def half(self, number, i):
            rows, cols = self.halves[i]
            start, size = (i * self.rows // 2, self.rows // 2) if self.is_tall else (0, self.rows)
            return self.mine.at[pl.ds(pl.multiple_of(number * self.rows + start, 16), size), cols]

        def to_sibling(self, j):
            return send(self.block(place.sibling_block(j)), self.sib.at[j], sems, (self.k, j), sibling)

        def in_transit(self, i):
            return send(self.half(place.block(2), i), self.transit[i], sems, (self.k, 4 + i), place.block(1 - 2 * i))

        def to_end(self, i, j):
            return send(self.half(place.block(1 - 2 * i), j), self.end[i].at[self.halves[j]], sems, (self.k, (8 if i == j else 6) + i), place.block(1 - 2 * i))

        def start(self):
            for j in (2, 1, 3, 0):
                self.to_sibling(j).start()

        def first(self):
            for j in (2, 1, 3, 0):
                self.to_sibling(j).wait_recv()
                mine, theirs = self.block(place.block(j)), self.sib.at[j]

                def add(rows, _):
                    mine[rows, :] = (mine[rows, :].astype(F32) + theirs[rows, :].astype(F32)).astype(BF16)

                each_row(self.rows, add)
                if j == 2:
                    for i in (0, 1):
                        self.in_transit(i).start()
                if j in (1, 3):
                    i = j // 2
                    self.to_end(i, 1 - i).start()

        def second(self):
            for i in (0, 1):
                self.in_transit(i).wait_recv()
                mine, theirs = self.half(place.block(1 - 2 * i), i), self.transit[i]

                def add(rows, _):
                    mine[rows, :] = (mine[rows, :].astype(F32) + theirs[rows, :].astype(F32)).astype(BF16)

                each_row(mine.shape[0], add)
                self.to_end(i, i).start()

        def last(self):
            for i in (0, 1):
                for j in (0, 1):
                    self.to_end(i, j).wait_recv()
            mine = self.block(me)

            def add(rows, total):
                g = (mine[rows, :].astype(F32) + self.end[0][rows, :].astype(F32) + self.end[1][rows, :].astype(F32)).astype(BF16)
                self.out[rows, :] = g
                g = g.astype(F32)
                return total + g[:8] * g[:8] + g[8:] * g[8:]

            cols = mine.shape[1]
            square = lax.fori_loop(0, self.rows // 16, lambda i, c: add(pl.ds(pl.multiple_of(i * 16, 16), 16), c), jnp.zeros((8, cols), F32))
            for c in chunks(cols, 128):
                part[...] += square[:, c]
            for j in (2, 1, 3, 0):
                self.to_sibling(j).wait_send()
            for i in (0, 1):
                self.in_transit(i).wait_send()
                for j in (0, 1):
                    self.to_end(i, j).wait_send()

    sums = [Sum(k) for k in range(6)]
    for k in range(4):
        pl.when(step == per * (k + 2) + 2)(sums[k].last)
    for k in range(5):
        pl.when(step == per * (k + 1) + 2)(sums[k].first)
        pl.when(step == per * (k + 2) - 1)(sums[k].second)

    @pl.when(which % 3 == 0)
    def _():
        tall[pl.ds(pl.multiple_of(tile * TILE, TILE), TILE), :] = dot(at[...], b[...]).T.astype(BF16)

    @pl.when(which % 3 != 0)
    def _():
        wide[which % 3 - 1, :, pl.ds(pl.multiple_of(tile * TILE, TILE), TILE)] = dot(at[...], b[...]).astype(BF16)

    for k in range(6):
        pl.when(step == per * (k + 1) - 1)(sums[k].start)

    @pl.when(step == per * 6 - 1)
    def _():
        sums[5].first()
        sums[4].last()
        sums[5].second()
        sums[5].last()
        exchange = [send(part, totals.at[j], sems, (6, j), peer) for j, peer in enumerate(peers)]
        for copy in exchange:
            copy.start()
        total = part[...]
        for copy in exchange:
            copy.wait_recv()
        for j in range(len(peers)):
            total += totals[j]
        out_total[...] = total
        for copy in exchange:
            copy.wait_send()


def summed_gradients(at, b, devices):
    (_, d, t), f = at.shape, b.shape[2]
    low, high, per = d // devices, f // devices, f // TILE
    vmem = pltpu.VMEM
    whole = lambda *shape: pl.BlockSpec(shape, lambda i: (0,) * len(shape))
    operand = lambda i: ((i // per % 3 + 1) // 2 + 2 * (i // per // 3), 0, 0)
    return pl.pallas_call(
        functools.partial(grads_kernel, devices),
        grid=(6 * per,),
        in_specs=[pl.BlockSpec((pl.squeezed, d, t), operand), pl.BlockSpec((pl.squeezed, t, TILE), lambda i: (i // per, 0, i % per))],
        out_specs=[whole(4, low, f), whole(2, high, d), whole(8, 128)],
        out_shape=[jax.ShapeDtypeStruct((4, low, f), BF16), jax.ShapeDtypeStruct((2, high, d), BF16), jax.ShapeDtypeStruct((8, 128), F32)],
        scratch_shapes=[
            vmem((2, d, f), BF16), vmem((f, d), BF16), vmem((2, 4, low, f), BF16), vmem((4, high, d), BF16),
            vmem((4, 2, low, f // 2), BF16), vmem((2, 2, high // 2, d), BF16), vmem((4, 2, low, f), BF16), vmem((2, 2, high, d), BF16),
            vmem((8, 128), F32), vmem((devices - 1, 8, 128), F32),
            pltpu.SemaphoreType.DMA((7, 10)), pltpu.SemaphoreType.DMA((7, 10)),
        ],
        compiler_params=pltpu.CompilerParams(vmem_limit_bytes=VMEM_LIMIT, collective_id=0, has_side_effects=True),
        cost_estimate=pl.CostEstimate(flops=12 * t * d * f, bytes_accessed=80 * 2**20, transcendentals=0),
        name="grads",
    )(at, b)


def gather_kernel(devices, *refs):
    count = (len(refs) - 3) // 2
    own, full, (local, sends, recvs) = refs[:count], refs[count : 2 * count], refs[2 * count :]
    place = Place(devices)
    me, right, left, sibling = place.me, place.block(1), place.block(3), place.sibling_block(0)
    place.barrier([right, left, sibling])
    pieces = [(a, n) for n in (0, 1) for a in range(count)]

    class Piece:
        def __init__(self, k):
            self.k = k
            self.a, self.n = pieces[k]
            self.rows = own[self.a].shape[1]
            self.by_rows = own[self.a].shape[1] > 128
            self.mine = own[self.a].at[self.n]

        def at(self, number):
            return full[self.a].at[self.n, pl.ds(pl.multiple_of(number * self.rows, 16), self.rows), :]

        def half(self, number, i):
            if self.by_rows:
                size = self.rows // 2
                return full[self.a].at[self.n, pl.ds(pl.multiple_of(number * self.rows + i * size, 16), size), :]
            size = full[self.a].shape[2] // 2
            return full[self.a].at[self.n, pl.ds(pl.multiple_of(number * self.rows, 16), self.rows), pl.ds(i * size, size)]

        def to(self, i):
            return send(self.mine, self.at(me), (sends, recvs), (self.k, i), (right, left, sibling)[i])

        def came(self, i):
            block = self.at((left, right, sibling)[i])
            return send(block, block, (sends, recvs), (self.k, i), sibling)

        def on(self, i):
            block = self.half((left, right)[i], i)
            return send(block, block, (sends, recvs), (self.k, 3 + i), (right, left)[i])

        def opposite(self, i):
            block = self.half(place.block(2), i)
            return send(block, block, (sends, recvs), (self.k, 3 + i), sibling)

        def across(self, i):
            block = self.at((left, right)[i]) if i < 2 else self.half(place.block(2), i - 2)
            return send(block, block, (sends, recvs), (self.k, 5 + i), sibling)

        def came_across(self, i):
            step = (3, 1, 2, 2)[i]
            block = self.at(place.sibling_block(step)) if i < 2 else self.half(place.sibling_block(2), i - 2)
            return send(block, block, (sends, recvs), (self.k, 5 + i), sibling)

        def keep(self):
            return pltpu.make_async_copy(self.mine, self.at(me), local.at[self.k])

        def start(self):
            for i in range(3):
                self.to(i).start()
            self.keep().start()

        def relay(self):
            for i in (0, 1):
                self.came(i).wait_recv()
                self.on(i).start()
                self.across(i).start()

        def finish(self):
            for i in (0, 1):
                self.opposite(i).wait_recv()
                self.across(2 + i).start()

        def end(self):
            self.keep().wait()
            self.came(2).wait_recv()
            for i in range(3):
                self.to(i).wait_send()
            for i in (0, 1):
                self.on(i).wait_send()
            for i in range(4):
                self.across(i).wait_send()
                self.came_across(i).wait_recv()

    work = [Piece(k) for k in range(len(pieces))]
    for k in range(2):
        work[k].start()
    for k in range(len(work)):
        work[k].relay()
        if k + 2 < len(work):
            work[k + 2].start()
        if k:
            work[k - 1].finish()
    work[-1].finish()
    for piece in work:
        piece.end()


def gathered(own, devices):
    return pl.pallas_call(
        functools.partial(gather_kernel, devices),
        in_specs=[pl.BlockSpec(memory_space=pltpu.VMEM)] * len(own),
        out_specs=[pl.BlockSpec(memory_space=pl.ANY)] * len(own),
        out_shape=[jax.ShapeDtypeStruct((w.shape[0], devices * w.shape[1], w.shape[2]), w.dtype) for w in own],
        scratch_shapes=[pltpu.SemaphoreType.DMA((6,)), pltpu.SemaphoreType.DMA((6, 9)), pltpu.SemaphoreType.DMA((6, 9))],
        compiler_params=pltpu.CompilerParams(vmem_limit_bytes=VMEM_LIMIT, collective_id=1, has_side_effects=True),
        name="gather",
    )(*own)


def adamw(w, m, v, g):
    m = 0.9 * m + 0.1 * g
    v = 0.95 * v + 0.05 * g * g
    step = m * lax.rsqrt(v + 1e-8) + 0.1 * w
    return (w - 0.02 * step).astype(BF16), m, v


def solution(mesh):
    devices = mesh.shape["dp"]

    def body(x, dy, wg, wu, wd, *moments):
        ms, vs = moments[:3], moments[3:]
        b, at = row_local(x[0], dy[0], wg, wu, wd)
        wide, tall, total = summed_gradients(at, b, devices)
        grads = [jnp.stack([wide[2], wide[0]]), jnp.stack([wide[3], wide[1]]), jnp.stack([tall[1], tall[0]])]
        factor = jnp.minimum(1.0, 0.5 * lax.rsqrt(jnp.sum(total) / sum(w.size for w in (wg, wu, wd)) + 1e-30))
        me = lax.axis_index("dp")
        new = []
        for w, m, v, g in zip((wg, wu, wd), ms, vs, grads, strict=True):
            own = lax.dynamic_slice_in_dim(w, me * m.shape[1], m.shape[1], 1).astype(F32)
            new.append(adamw(own, m, v, g.astype(F32) * factor))
        new_w, new_m, new_v = zip(*new, strict=True)
        return (*gathered(new_w, devices), *new_m, *new_v)

    data, whole, rows = P(("rep", "dp")), P(), P(None, "dp")
    return jax.shard_map(
        body,
        mesh=mesh,
        in_specs=(data, data, whole, whole, whole, *[rows] * 6),
        out_specs=(*[P("rep")] * 3, *[P("rep", "dp")] * 6),
        check_vma=False,
    )
```

```python
import functools

import jax
import jax.numpy as jnp
from jax import lax
from jax.experimental import pallas as pl
from jax.experimental.pallas import tpu as pltpu
from jax.sharding import PartitionSpec as P

F32, BF16 = jnp.float32, jnp.bfloat16
VMEM_LIMIT = 63 * 1024 * 1024
NT = (((1,), (1,)), ((), ()))
GRADS_LIMIT = 59 * 1024 * 1024
ROWS = 256


def dot(a, b, dims=(((1,), (0,)), ((), ()))):
    return lax.dot_general(a, b, dims, preferred_element_type=F32)


def scale_of(wide):
    return lax.rsqrt(jnp.mean(wide * wide, -1, keepdims=True) + 1e-6)


def normed(h):
    wide = h.astype(F32)
    return (wide * scale_of(wide)).astype(BF16)


def chunks(total, size):
    return [slice(at, min(at + size, total)) for at in range(0, total, size)]


def gated(gate, up, dact):
    s = jax.nn.sigmoid(gate)
    silu = gate * s
    return (dact * up * (s + silu * (1 - s))).astype(BF16), (dact * silu).astype(BF16)


def rows_kernel(x, dy, wg, wu, wd, b, at, gate0, up0, held_wide, held_down, arrived):
    order = [(wg.at[0], held_wide.at[0]), (wu.at[0], held_wide.at[1]), (wd.at[0], held_down.at[0])]
    order += [(wg.at[1], held_wide.at[2]), (wu.at[1], held_wide.at[3]), (wd.at[1], held_down.at[1])]
    copies = [pltpu.make_async_copy(src, dst, arrived.at[n]) for n, (src, dst) in enumerate(order)]
    first = pl.program_id(0) == 0

    @pl.when(first)
    def _():
        for copy in copies:
            copy.start()

    def need(*which):
        @pl.when(first)
        def _():
            for n in which:
                copies[n].wait()

    wg0, wu0, wd0, wg1, wu1, wd1 = (dst for _, dst in order)
    cols = chunks(wg.shape[2], 512)
    a = normed(x[...])
    at[3] = a.T
    d = dy[...]
    at[0] = d.T
    need(0, 1)
    for c in cols:
        gate, up = dot(a, wg0[:, c]), dot(a, wu0[:, c])
        gate0[:, c], up0[:, c] = gate, up
        b[4, :, c] = (jax.nn.silu(gate) * up).astype(BF16)
    need(2)
    h = x[...] + dot(b[4], wd0[...]).astype(BF16)
    a = normed(h)
    at[1] = a.T
    need(3, 4, 5)
    for c in cols:
        gate, up = dot(a, wg1[:, c]), dot(a, wu1[:, c])
        dact = dot(d, wd1[c, :], NT).astype(BF16).astype(F32)
        b[1, :, c] = (jax.nn.silu(gate) * up).astype(BF16)
        b[0, :, c], b[2, :, c] = gated(gate, up, dact)
    da = dot(b[0], wg1[...], NT).astype(BF16) + dot(b[2], wu1[...], NT).astype(BF16)
    da, wide = da.astype(F32), h.astype(F32)
    scale = scale_of(wide)
    inner = jnp.mean(da * wide, -1, keepdims=True)
    d = d + (da * scale - wide * (scale * scale * scale * inner)).astype(BF16)
    at[2] = d.T
    for c in cols:
        dact = dot(d, wd0[c, :], NT).astype(BF16).astype(F32)
        b[3, :, c], b[5, :, c] = gated(gate0[:, c], up0[:, c], dact)


def row_local(x, dy, wg, wu, wd):
    t, d = x.shape
    f = wg.shape[2]
    rows, anywhere = pl.BlockSpec((ROWS, d), lambda i: (i, 0)), pl.BlockSpec(memory_space=pl.ANY)
    return pl.pallas_call(
        rows_kernel,
        grid=(t // ROWS,),
        in_specs=[rows, rows] + [anywhere] * 3,
        out_specs=[pl.BlockSpec((6, ROWS, f), lambda i: (0, i, 0)), pl.BlockSpec((4, d, ROWS), lambda i: (0, 0, i))],
        out_shape=[jax.ShapeDtypeStruct((6, t, f), BF16), jax.ShapeDtypeStruct((4, d, t), BF16)],
        scratch_shapes=[
            pltpu.VMEM((ROWS, f), F32), pltpu.VMEM((ROWS, f), F32), pltpu.VMEM((4, d, f), BF16), pltpu.VMEM((2, f, d), BF16),
            pltpu.SemaphoreType.DMA((6,)),
        ],
        compiler_params=pltpu.CompilerParams(vmem_limit_bytes=VMEM_LIMIT),
        cost_estimate=pl.CostEstimate(flops=18 * t * d * f, bytes_accessed=150 * 2**20, transcendentals=0),
        name="rows",
    )(x, dy, wg, wu, wd)


class Place:
    def __init__(self, devices):
        assert devices == 8
        self.devices = devices
        self.me = lax.axis_index("dp")
        self.chip, self.core = self.me // 2, self.me % 2

    def block(self, step):
        return (self.chip + step) % 4 * 2 + self.core

    def sibling_block(self, step):
        return (self.chip + step) % 4 * 2 + 1 - self.core

    def barrier(self, peers):
        semaphore = pltpu.get_barrier_semaphore()
        for peer in peers:
            pl.semaphore_signal(semaphore, inc=1, device_id={"dp": peer}, device_id_type=pl.DeviceIdType.MESH)
        pl.semaphore_wait(semaphore, len(peers))


def send(src, dst, sems, at, to):
    return pltpu.make_async_remote_copy(
        src_ref=src, dst_ref=dst, send_sem=sems[0].at[at], recv_sem=sems[1].at[at], device_id={"dp": to}, device_id_type=pl.DeviceIdType.MESH
    )


def each_row(count, body, size=16):
    lax.fori_loop(0, count // size, lambda i, c: body(pl.ds(pl.multiple_of(i * size, size), size), c) or c, 0)


def grads_kernel(
    devices, at, b, out_wide, out_tall, out_total, wide, tall, sib_wide, sib_tall, transit_wide, transit_tall, end_wide, end_tall, part, totals, sends, recvs
):
    step = pl.program_id(0)
    which, side = step // 2, step % 2
    place = Place(devices)
    me = place.me
    peers = [(me + j) % devices for j in range(1, devices)]
    sibling = place.sibling_block(0)
    sems = (sends, recvs)
    low, high = wide.shape[1] // devices, tall.shape[0] // devices
    width = wide.shape[2]

    @pl.when(step == 0)
    def _():
        part[...] = jnp.zeros_like(part)
        place.barrier(peers)

    class Sum:
        def __init__(self, number, k, part):
            self.number, n = number, k // 3
            self.is_tall = k % 3 == 1
            self.ready = 4 * (k + 1) - (2 if part == 0 else 0)
            if self.is_tall:
                self.rows, self.cols, self.mine, self.sib = high, slice(None), tall, sib_tall
                self.transit, self.end, self.out = [transit_tall.at[n, i] for i in (0, 1)], [end_tall.at[n, i] for i in (0, 1)], out_tall.at[n]
                self.halves = [(pl.ds(i * high // 2, high // 2), slice(None)) for i in (0, 1)]
            else:
                slot = k % 3 // 2
                at = 2 * n + slot
                start, size = (0, width) if part is None else (part * width // 2, width // 2)
                self.rows, self.cols, self.mine, self.sib = low, pl.ds(start, size), wide.at[slot], sib_wide.at[slot]
                c = size // 2
                self.transit = [transit_wide.at[at, i, :, pl.ds(start // 2, c)] for i in (0, 1)]
                self.end, self.out = [end_wide.at[at, i] for i in (0, 1)], out_wide.at[at]
                self.halves = [(slice(None), pl.ds(start + i * c, c)) for i in (0, 1)]

        def block(self, number):
            return self.mine.at[pl.ds(pl.multiple_of(number * self.rows, 16), self.rows), self.cols]

        def half(self, number, i):
            start, size = (i * self.rows // 2, self.rows // 2) if self.is_tall else (0, self.rows)
            return self.mine.at[pl.ds(pl.multiple_of(number * self.rows + start, 16), size), self.halves[i][1]]

        def theirs(self, j):
            return self.sib.at[j, :, self.cols]

        def to_sibling(self, j):
            return send(self.block(place.sibling_block(j)), self.theirs(j), sems, (self.number, j), sibling)

        def in_transit(self, i):
            return send(self.half(place.block(2), i), self.transit[i], sems, (self.number, 4 + i), place.block(1 - 2 * i))

        def to_end(self, i, j):
            copy = (8 if i == j else 6) + i
            return send(self.half(place.block(1 - 2 * i), j), self.end[i].at[self.halves[j]], sems, (self.number, copy), place.block(1 - 2 * i))

        def start(self):
            for j in (2, 1, 3, 0):
                self.to_sibling(j).start()

        def add(self, mine, theirs):
            def add(rows, _):
                mine[rows, :] = (mine[rows, :].astype(F32) + theirs[rows, :].astype(F32)).astype(BF16)

            each_row(mine.shape[0], add)

        def first(self):
            for j in (2, 1, 3, 0):
                self.to_sibling(j).wait_recv()
                self.add(self.block(place.block(j)), self.theirs(j))
                if j == 2:
                    for i in (0, 1):
                        self.in_transit(i).start()
                if j in (1, 3):
                    self.to_end(j // 2, 1 - j // 2).start()

        def second(self):
            for i in (0, 1):
                self.in_transit(i).wait_recv()
                self.add(self.half(place.block(1 - 2 * i), i), self.transit[i])
                self.to_end(i, i).start()

        def last(self):
            for i in (0, 1):
                for j in (0, 1):
                    self.to_end(i, j).wait_recv()
            mine, out = self.block(me), self.out.at[:, self.cols]
            ends = [end.at[:, self.cols] for end in self.end]

            def add(rows, total):
                g = (mine[rows, :].astype(F32) + ends[0][rows, :].astype(F32) + ends[1][rows, :].astype(F32)).astype(BF16)
                out[rows, :] = g
                g = g.astype(F32)
                return total + g[:8] * g[:8] + g[8:] * g[8:]

            cols = mine.shape[1]
            square = lax.fori_loop(0, self.rows // 16, lambda i, c: add(pl.ds(pl.multiple_of(i * 16, 16), 16), c), jnp.zeros((8, cols), F32))
            for c in chunks(cols, 128):
                part[...] += square[:, c]
            for j in (2, 1, 3, 0):
                self.to_sibling(j).wait_send()
            for i in (0, 1):
                self.in_transit(i).wait_send()
                for j in (0, 1):
                    self.to_end(i, j).wait_send()

    sums = [Sum(n, *of) for n, of in enumerate(((0, 0), (0, 1), (1, None), (2, None), (3, None), (4, None), (5, 0), (5, 1)))]
    moves = []
    for n, one in enumerate(sums):
        after = sums[n + 1].ready + 3 if n + 1 < len(sums) else one.ready + 4
        moves += [(one.ready, 0, one.start), (one.ready + 1, 1, one.first), (one.ready + 3, 2, one.second), (after, 3, one.last)]
    moves.sort(key=lambda move: move[:2])

    def at_point(point):
        for due, _, move in moves:
            if due % 2 == point and due < 24:
                pl.when(step == due // 2)(move)

    def compute(start, size):
        cols = pl.ds(start, size)

        @pl.when(which % 3 == 1)
        def _():
            tall[pl.ds(pl.multiple_of(side * (width // 2) + start, 256), size), :] = dot(at[...], b[:, cols]).astype(BF16).T

        @pl.when(which % 3 != 1)
        def _():
            wide[which % 3 // 2, :, pl.ds(pl.multiple_of(side * (width // 2) + start, 256), size)] = dot(at[...], b[:, cols]).astype(BF16)

    at_point(0)
    compute(0, 512)
    at_point(1)
    compute(512, width // 2 - 512)

    @pl.when(step == 11)
    def _():
        for due, _, move in moves:
            if due >= 24:
                move()
        exchange = [send(part, totals.at[j], sems, (8, j), peer) for j, peer in enumerate(peers)]
        for copy in exchange:
            copy.start()
        total = part[...]
        for copy in exchange:
            copy.wait_recv()
        for j in range(len(peers)):
            total += totals[j]
        out_total[...] = total
        for copy in exchange:
            copy.wait_send()


def summed_gradients(at, b, devices):
    (_, d, t), f = at.shape, b.shape[2]
    low, high = d // devices, f // devices
    vmem = pltpu.VMEM
    whole = pl.BlockSpec(memory_space=vmem)
    operand = lambda i: (2 * (i // 6) + 1 - i // 2 % 3 % 2, 0, 0)
    return pl.pallas_call(
        functools.partial(grads_kernel, devices),
        grid=(12,),
        in_specs=[pl.BlockSpec((pl.squeezed, d, t), operand), pl.BlockSpec((pl.squeezed, t, f // 2), lambda i: (i // 2, 0, i % 2))],
        out_specs=[whole] * 3,
        out_shape=[vmem((4, low, f), BF16), vmem((2, high, d), BF16), vmem((8, 128), F32)],
        scratch_shapes=[
            vmem((2, d, f), BF16), vmem((f, d), BF16), vmem((2, 4, low, f), BF16), vmem((4, high, d), BF16),
            vmem((4, 2, low, f // 2), BF16), vmem((2, 2, high // 2, d), BF16), vmem((4, 2, low, f), BF16), vmem((2, 2, high, d), BF16),
            vmem((8, 128), F32), vmem((devices - 1, 8, 128), F32),
            pltpu.SemaphoreType.DMA((9, 10)), pltpu.SemaphoreType.DMA((9, 10)),
        ],
        compiler_params=pltpu.CompilerParams(vmem_limit_bytes=GRADS_LIMIT, collective_id=0, has_side_effects=True),
        cost_estimate=pl.CostEstimate(flops=12 * t * d * f, bytes_accessed=80 * 2**20, transcendentals=0),
        name="grads",
    )(at, b)


def adamw(w, m, v, g):
    m = 0.9 * m + 0.1 * g
    v = 0.95 * v + 0.05 * g * g
    step = m * lax.rsqrt(v + 1e-8) + 0.1 * w
    return (w - 0.02 * step).astype(BF16), m, v


class Piece:
    def __init__(self, k, place, layer, full, m, v, w_from, m_from, v_from, g, loads, sems):
        self.k, self.place, self.layer, self.full = k, place, layer, full
        self.m, self.v, self.g, self.sems, self.loads = m.at[layer], v.at[layer], g, sems, loads
        self.w_from, self.m_from, self.v_from = w_from, m_from.at[layer], v_from.at[layer]
        self.rows, self.cols = m.shape[1:]
        self.me, self.right, self.left, self.sibling = place.me, place.block(1), place.block(3), place.sibling_block(0)

    def at(self, number, of=None):
        return (self.full if of is None else of).at[self.layer, pl.ds(pl.multiple_of(number * self.rows, 16), self.rows), :]

    def half(self, number, i):
        if self.rows % 32:
            size = self.cols // 2
            return self.full.at[self.layer, pl.ds(pl.multiple_of(number * self.rows, 16), self.rows), pl.ds(i * size, size)]
        size = self.rows // 2
        return self.full.at[self.layer, pl.ds(pl.multiple_of(number * self.rows + i * size, 16), size), :]

    def load(self):
        pairs = ((self.at(self.me, self.w_from), self.at(self.me)), (self.m_from, self.m), (self.v_from, self.v))
        return [pltpu.make_async_copy(src, dst, self.loads.at[self.k, i]) for i, (src, dst) in enumerate(pairs)]

    def update(self, factor):
        w_ref = self.at(self.me)
        for copy in self.load():
            copy.wait()

        def chunk(rows, _):
            w, m, v = adamw(w_ref[rows, :].astype(F32), self.m[rows, :], self.v[rows, :], self.g[rows, :].astype(F32) * factor)
            w_ref[rows, :], self.m[rows, :], self.v[rows, :] = w, m, v

        each_row(self.rows, chunk)

    def copy(self, ref, number, to):
        return send(ref, ref, self.sems, (self.k, number), to)

    def own(self, i):
        return self.copy(self.at(self.me), i, (self.right, self.left, self.sibling)[i])

    def came(self, i):
        return self.copy(self.at((self.left, self.right, self.sibling)[i]), i, self.sibling)

    def on(self, i):
        return self.copy(self.half((self.left, self.right)[i], i), 3 + i, (self.right, self.left)[i])

    def opposite(self, i):
        return self.copy(self.half(self.place.block(2), i), 3 + i, self.sibling)

    def across(self, i):
        return self.copy(self.at((self.left, self.right)[i]) if i < 2 else self.half(self.place.block(2), i - 2), 5 + i, self.sibling)

    def came_across(self, i):
        of = self.place.sibling_block
        return self.copy(self.at(of((3, 1)[i])) if i < 2 else self.half(of(2), i - 2), 5 + i, self.sibling)

    def start(self):
        for i in range(3):
            self.own(i).start()

    def relay(self):
        for i in (0, 1):
            self.came(i).wait_recv()
            self.on(i).start()
            self.across(i).start()

    def finish(self):
        for i in (0, 1):
            self.opposite(i).wait_recv()
            self.across(2 + i).start()

    def end(self):
        self.came(2).wait_recv()
        for i in range(3):
            self.own(i).wait_send()
        for i in (0, 1):
            self.on(i).wait_send()
        for i in range(4):
            self.across(i).wait_send()
            self.came_across(i).wait_recv()


def update_kernel(devices, wide, tall, total, *refs):
    ws, ms, vs, full, new_m, new_v, (loads, sends, recvs) = (refs[i : i + 3] for i in range(0, 21, 3))
    place = Place(devices)
    work = []
    for k in range(6):
        a, layer = (k + 2) % 3, 1 - k // 3
        g = tall.at[1 - layer] if a == 2 else wide.at[2 * (1 - layer) + a]
        work.append(Piece(k, place, layer, full[a], new_m[a], new_v[a], ws[a], ms[a], vs[a], g, loads, (sends, recvs)))
    for piece in work:
        for copy in piece.load():
            copy.start()
    place.barrier([place.block(1), place.block(3), place.sibling_block(0)])
    count = sum(w.shape[0] * w.shape[1] * w.shape[2] for w in ws)
    factor = jnp.minimum(1.0, 0.5 * lax.rsqrt(jnp.sum(total[...], keepdims=True) / count + 1e-30))
    for piece in work:
        piece.update(factor)
        piece.start()
    for k, piece in enumerate(work):
        piece.relay()
        if k:
            work[k - 1].finish()
    work[-1].finish()
    for piece in work:
        piece.end()


def store_kernel(*refs):
    count = len(refs) // 2
    copies = [pltpu.make_async_copy(refs[i], refs[count + i], refs[-1].at[i]) for i in range(count)]
    for copy in copies:
        copy.start()
    for copy in copies:
        copy.wait()


def updated(wide, tall, total, ws, ms, vs, devices):
    out = [*ws, *ms, *vs]
    anywhere, vmem = pl.BlockSpec(memory_space=pl.ANY), pl.BlockSpec(memory_space=pltpu.VMEM)
    new = pl.pallas_call(
        functools.partial(update_kernel, devices),
        in_specs=[vmem] * 3 + [anywhere] * 9,
        out_specs=[vmem] * 9,
        out_shape=[pltpu.VMEM(o.shape, o.dtype) for o in out],
        scratch_shapes=[pltpu.SemaphoreType.DMA((6, 3)), pltpu.SemaphoreType.DMA((6, 9)), pltpu.SemaphoreType.DMA((6, 9))],
        compiler_params=pltpu.CompilerParams(vmem_limit_bytes=4 * 1024 * 1024, collective_id=1, has_side_effects=True),
        name="update",
    )(*[pltpu.with_memory_space_constraint(g, pltpu.VMEM) for g in (wide, tall, total)], *[pltpu.with_memory_space_constraint(o, pltpu.HBM) for o in out])
    return pl.pallas_call(
        store_kernel,
        in_specs=[vmem] * 9,
        out_specs=[anywhere] * 9,
        out_shape=[jax.ShapeDtypeStruct(o.shape, o.dtype) for o in out],
        scratch_shapes=[pltpu.SemaphoreType.DMA((9,))],
        compiler_params=pltpu.CompilerParams(vmem_limit_bytes=1024 * 1024),
        name="store",
    )(*[pltpu.with_memory_space_constraint(n, pltpu.VMEM) for n in new])


def solution(mesh):
    devices = mesh.shape["dp"]

    def body(x, dy, wg, wu, wd, *moments):
        b, at = row_local(x[0], dy[0], wg, wu, wd)
        wide, tall, total = summed_gradients(at, b, devices)
        return tuple(updated(wide, tall, total, (wg, wu, wd), moments[:3], moments[3:], devices))

    data, whole, rows = P(("rep", "dp")), P(), P(None, "dp")
    return jax.shard_map(
        body,
        mesh=mesh,
        in_specs=(data, data, whole, whole, whole, *[rows] * 6),
        out_specs=(*[P("rep")] * 3, *[P("rep", "dp")] * 6),
        check_vma=False,
    )
```

```python
import functools

import jax
import jax.numpy as jnp
from jax import lax
from jax.experimental import pallas as pl
from jax.experimental.pallas import tpu as pltpu
from jax.sharding import PartitionSpec as P

F32, BF16 = jnp.float32, jnp.bfloat16
VMEM_LIMIT = 63 * 1024 * 1024
NT = (((1,), (1,)), ((), ()))
GRADS_LIMIT = 59 * 1024 * 1024
PART = 512
ROWS = 256


def dot(a, b, dims=(((1,), (0,)), ((), ()))):
    return lax.dot_general(a, b, dims, preferred_element_type=F32)


def scale_of(wide):
    return lax.rsqrt(jnp.mean(wide * wide, -1, keepdims=True) + 1e-6)


def normed(h):
    wide = h.astype(F32)
    return (wide * scale_of(wide)).astype(BF16)


def chunks(total, size):
    return [slice(at, min(at + size, total)) for at in range(0, total, size)]


def gated(gate, up, dact):
    s = jax.nn.sigmoid(gate)
    silu = gate * s
    return (dact * up * (s + silu * (1 - s))).astype(BF16), (dact * silu).astype(BF16)


def rows_kernel(x, dy, wg, wu, wd, b, at, gate0, up0, held_wide, held_down, arrived):
    order = [(wg.at[0], held_wide.at[0]), (wu.at[0], held_wide.at[1]), (wd.at[0], held_down.at[0])]
    order += [(wg.at[1], held_wide.at[2]), (wu.at[1], held_wide.at[3]), (wd.at[1], held_down.at[1])]
    copies = [pltpu.make_async_copy(src, dst, arrived.at[n]) for n, (src, dst) in enumerate(order)]
    wg0, wu0, wd0, wg1, wu1, wd1 = (dst for _, dst in order)
    cols = chunks(wg.shape[2], 512)

    def tile(need):
        a = normed(x[...])
        at[3] = a.T
        d = dy[...]
        at[0] = d.T
        need(0, 1)
        for c in cols:
            gate, up = dot(a, wg0[:, c]), dot(a, wu0[:, c])
            gate0[:, c], up0[:, c] = gate, up
            b[4, :, c] = (jax.nn.silu(gate) * up).astype(BF16)
        need(2)
        h = x[...] + dot(b[4], wd0[...]).astype(BF16)
        a = normed(h)
        at[1] = a.T
        need(3, 4, 5)
        for c in cols:
            gate, up = dot(a, wg1[:, c]), dot(a, wu1[:, c])
            dact = dot(d, wd1[c, :], NT).astype(BF16).astype(F32)
            b[2, :, c] = (jax.nn.silu(gate) * up).astype(BF16)
            b[0, :, c], b[1, :, c] = gated(gate, up, dact)
        da = (dot(wg1[...], b[0], NT).astype(BF16) + dot(wu1[...], b[1], NT).astype(BF16)).T
        da, wide = da.astype(F32), h.astype(F32)
        scale = scale_of(wide)
        inner = jnp.mean(da * wide, -1, keepdims=True)
        d = d + (da * scale - wide * (scale * scale * scale * inner)).astype(BF16)
        at[2] = d.T
        for c in cols:
            dact = dot(d, wd0[c, :], NT).astype(BF16).astype(F32)
            b[3, :, c], b[5, :, c] = gated(gate0[:, c], up0[:, c], dact)

    first = pl.program_id(0) == 0

    @pl.when(first)
    def _():
        for copy in copies:
            copy.start()

        def need(*which):
            for n in which:
                copies[n].wait()

        tile(need)

    @pl.when(jnp.logical_not(first))
    def _():
        tile(lambda *which: None)


def row_local(x, dy, wg, wu, wd):
    t, d = x.shape
    f = wg.shape[2]
    rows, anywhere = pl.BlockSpec((ROWS, d), lambda i: (i, 0)), pl.BlockSpec(memory_space=pl.ANY)
    return pl.pallas_call(
        rows_kernel,
        grid=(t // ROWS,),
        in_specs=[rows, rows] + [anywhere] * 3,
        out_specs=[pl.BlockSpec((6, ROWS, f), lambda i: (0, i, 0)), pl.BlockSpec((4, d, ROWS), lambda i: (0, 0, i))],
        out_shape=[jax.ShapeDtypeStruct((6, t, f), BF16), jax.ShapeDtypeStruct((4, d, t), BF16)],
        scratch_shapes=[
            pltpu.VMEM((ROWS, f), F32), pltpu.VMEM((ROWS, f), F32), pltpu.VMEM((4, d, f), BF16), pltpu.VMEM((2, f, d), BF16),
            pltpu.SemaphoreType.DMA((6,)),
        ],
        compiler_params=pltpu.CompilerParams(vmem_limit_bytes=VMEM_LIMIT),
        cost_estimate=pl.CostEstimate(flops=18 * t * d * f, bytes_accessed=150 * 2**20, transcendentals=0),
        name="rows",
    )(x, dy, wg, wu, wd)


class Place:
    def __init__(self, devices):
        assert devices == 8
        self.devices = devices
        self.me = lax.axis_index("dp")
        self.chip, self.core = self.me // 2, self.me % 2

    def block(self, step):
        return (self.chip + step) % 4 * 2 + self.core

    def sibling_block(self, step):
        return (self.chip + step) % 4 * 2 + 1 - self.core

    def barrier(self, peers):
        semaphore = pltpu.get_barrier_semaphore()
        for peer in peers:
            pl.semaphore_signal(semaphore, inc=1, device_id={"dp": peer}, device_id_type=pl.DeviceIdType.MESH)
        pl.semaphore_wait(semaphore, len(peers))


def send(src, dst, sems, at, to):
    return pltpu.make_async_remote_copy(
        src_ref=src, dst_ref=dst, send_sem=sems[0].at[at], recv_sem=sems[1].at[at], device_id={"dp": to}, device_id_type=pl.DeviceIdType.MESH
    )


def each_row(count, body, size=16):
    lax.fori_loop(0, count // size, lambda i, c: body(pl.ds(pl.multiple_of(i * size, size), size), c) or c, 0)


def grads_kernel(
    devices, at, b, out_wide, out_tall, out_total, wide, tall, sib_wide, sib_tall, transit_wide, transit_tall, end_wide, end_tall, part, totals, sends, recvs
):
    step = pl.program_id(0)
    which, side = step // 2, step % 2
    place = Place(devices)
    me = place.me
    peers = [(me + j) % devices for j in range(1, devices)]
    sibling = place.sibling_block(0)
    sems = (sends, recvs)
    low, high = wide.shape[1] // devices, tall.shape[1] // devices
    width = wide.shape[2]

    @pl.when(step == 0)
    def _():
        part[...] = jnp.zeros_like(part)
        place.barrier(peers)

    class Sum:
        def __init__(self, number, k, ready, start=0, size=None):
            self.number, n = number, k // 3
            self.is_tall, self.ready = k in (2, 4), ready
            self.end_by = (12, 20, 26, 26, 28, 28 + number % 2)[k]
            size = size or width
            if self.is_tall:
                self.rows, self.cols, self.mine, self.sib = high, slice(None), tall.at[n], sib_tall.at[n]
                self.transit, self.end, self.out = [transit_tall.at[n, i] for i in (0, 1)], [end_tall.at[n, i] for i in (0, 1)], out_tall.at[n]
                self.halves = [(pl.ds(i * high // 2, high // 2), slice(None)) for i in (0, 1)]
            else:
                slot = (k % 3 + 1) // 2
                at = 2 * n + slot
                self.rows, self.cols, self.mine, self.sib = low, pl.ds(start, size), wide.at[slot], sib_wide.at[slot]
                c = size // 2
                self.transit = [transit_wide.at[at, i, :, pl.ds(start // 2, c)] for i in (0, 1)]
                self.end, self.out = [end_wide.at[at, i] for i in (0, 1)], out_wide.at[at]
                self.halves = [(slice(None), pl.ds(start + i * c, c)) for i in (0, 1)]

        def block(self, number):
            return self.mine.at[pl.ds(pl.multiple_of(number * self.rows, 16), self.rows), self.cols]

        def half(self, number, i):
            start, size = (i * self.rows // 2, self.rows // 2) if self.is_tall else (0, self.rows)
            return self.mine.at[pl.ds(pl.multiple_of(number * self.rows + start, 16), size), self.halves[i][1]]

        def theirs(self, j):
            return self.sib.at[j, :, self.cols]

        def to_sibling(self, j):
            return send(self.block(place.sibling_block(j)), self.theirs(j), sems, (self.number, j), sibling)

        def in_transit(self, i):
            return send(self.half(place.block(2), i), self.transit[i], sems, (self.number, 4 + i), place.block(1 - 2 * i))

        def to_end(self, i, j):
            copy = (8 if i == j else 6) + i
            return send(self.half(place.block(1 - 2 * i), j), self.end[i].at[self.halves[j]], sems, (self.number, copy), place.block(1 - 2 * i))

        def start(self):
            for j in (2, 1, 3, 0):
                self.to_sibling(j).start()

        def add(self, mine, theirs):
            def add(rows, _):
                mine[rows, :] = (mine[rows, :].astype(F32) + theirs[rows, :].astype(F32)).astype(BF16)

            each_row(mine.shape[0], add)

        def first(self):
            for j in (2, 1, 3, 0):
                self.to_sibling(j).wait_recv()
                self.add(self.block(place.block(j)), self.theirs(j))
                if j == 2:
                    for i in (0, 1):
                        self.in_transit(i).start()
                if j in (1, 3):
                    self.to_end(j // 2, 1 - j // 2).start()

        def second(self):
            for i in (0, 1):
                self.in_transit(i).wait_recv()
                self.add(self.half(place.block(1 - 2 * i), i), self.transit[i])
                self.to_end(i, i).start()

        def last(self):
            for i in (0, 1):
                for j in (0, 1):
                    self.to_end(i, j).wait_recv()
            mine, out = self.block(me), self.out.at[:, self.cols]
            ends = [end.at[:, self.cols] for end in self.end]

            def add(rows, total):
                g = (mine[rows, :].astype(F32) + ends[0][rows, :].astype(F32) + ends[1][rows, :].astype(F32)).astype(BF16)
                out[rows, :] = g
                g = g.astype(F32)
                return total + g[:8] * g[:8] + g[8:] * g[8:]

            cols = mine.shape[1]
            square = lax.fori_loop(0, self.rows // 16, lambda i, c: add(pl.ds(pl.multiple_of(i * 16, 16), 16), c), jnp.zeros((8, cols), F32))
            for c in chunks(cols, 128):
                part[...] += square[:, c]
            for j in (2, 1, 3, 0):
                self.to_sibling(j).wait_send()
            for i in (0, 1):
                self.in_transit(i).wait_send()
                for j in (0, 1):
                    self.to_end(i, j).wait_send()

    half = width // 2
    parts = [(0, 1, 0, PART), (0, 2, PART, half - PART), (0, 4, half, half), (1, 6, 0, half), (1, 8, half, half)]
    parts += [(2, 12), (3, 16), (4, 20), (5, 22, 0, half), (5, 24, half, half)]
    sums = [Sum(n, *of) for n, of in enumerate(parts)]
    moves = []
    for n, one in enumerate(sums):
        moves += [(one.ready, 0, one.start), (one.ready + 1, 1, one.first), (one.ready + (2 if n == 1 else 3), 2, one.second), (one.end_by, 3, one.last)]
    moves.sort(key=lambda move: move[:2])

    def at_point(point):
        for due, _, move in moves:
            if due % 2 == point and due < 24:
                pl.when(step == due // 2)(move)

    def compute(start, size):
        cols = pl.ds(start, size)

        is_tall = (which % 2 == 0) & (which > 0)

        @pl.when(is_tall)
        def _():
            tall[which // 2 - 1, pl.ds(pl.multiple_of(side * half + start, 256), size), :] = dot(at[...], b[:, cols]).astype(BF16).T

        @pl.when(jnp.logical_not(is_tall))
        def _():
            wide[(which % 3 + 1) // 2, :, pl.ds(pl.multiple_of(side * half + start, 256), size)] = dot(at[...], b[:, cols]).astype(BF16)

    at_point(0)
    compute(0, PART)
    at_point(1)
    compute(PART, half - PART)

    @pl.when(step == 11)
    def _():
        for due, _, move in moves:
            if due >= 24:
                move()
        exchange = [send(part, totals.at[j], sems, (len(sums), j), peer) for j, peer in enumerate(peers)]
        for copy in exchange:
            copy.start()
        total = part[...]
        for copy in exchange:
            copy.wait_recv()
        for j in range(len(peers)):
            total += totals[j]
        out_total[...] = total
        for copy in exchange:
            copy.wait_send()


def summed_gradients(at, b, devices):
    (_, d, t), f = at.shape, b.shape[2]
    low, high = d // devices, f // devices
    vmem = pltpu.VMEM
    whole = pl.BlockSpec(memory_space=vmem)
    operand = lambda i: (2 * (i // 6) + 1 - (1 - i // 2 % 2) * ((i // 2 + 5) // 6), 0, 0)
    return pl.pallas_call(
        functools.partial(grads_kernel, devices),
        grid=(12,),
        in_specs=[pl.BlockSpec((pl.squeezed, d, t), operand), pl.BlockSpec((pl.squeezed, t, f // 2), lambda i: (i // 2, 0, i % 2))],
        out_specs=[whole] * 3,
        out_shape=[vmem((4, low, f), BF16), vmem((2, high, d), BF16), vmem((8, 128), F32)],
        scratch_shapes=[
            vmem((2, d, f), BF16), vmem((2, f, d), BF16), vmem((2, 4, low, f), BF16), vmem((2, 4, high, d), BF16),
            vmem((4, 2, low, f // 2), BF16), vmem((2, 2, high // 2, d), BF16), vmem((4, 2, low, f), BF16), vmem((2, 2, high, d), BF16),
            vmem((8, 128), F32), vmem((devices - 1, 8, 128), F32),
            pltpu.SemaphoreType.DMA((11, 10)), pltpu.SemaphoreType.DMA((11, 10)),
        ],
        compiler_params=pltpu.CompilerParams(vmem_limit_bytes=GRADS_LIMIT, collective_id=0, has_side_effects=True),
        cost_estimate=pl.CostEstimate(flops=12 * t * d * f, bytes_accessed=80 * 2**20, transcendentals=0),
        name="grads",
    )(at, b)


def adamw(w, m, v, g):
    m = 0.9 * m + 0.1 * g
    v = 0.95 * v + 0.05 * g * g
    step = m * lax.rsqrt(v + 1e-8) + 0.1 * w
    return (w - 0.02 * step).astype(BF16), m, v


class Piece:
    def __init__(self, k, place, layer, full, m, v, w_from, m_from, v_from, g, loads, sems):
        self.k, self.place, self.layer, self.full = k, place, layer, full
        self.m, self.v, self.g, self.sems, self.loads = m.at[layer], v.at[layer], g, sems, loads
        self.w_from, self.m_from, self.v_from = w_from, m_from.at[layer], v_from.at[layer]
        self.rows, self.cols = m.shape[1:]
        self.me, self.right, self.left, self.sibling = place.me, place.block(1), place.block(3), place.sibling_block(0)

    def at(self, number, of=None):
        return (self.full if of is None else of).at[self.layer, pl.ds(pl.multiple_of(number * self.rows, 16), self.rows), :]

    def half(self, number, i):
        if self.rows % 32:
            size = self.cols // 2
            return self.full.at[self.layer, pl.ds(pl.multiple_of(number * self.rows, 16), self.rows), pl.ds(i * size, size)]
        size = self.rows // 2
        return self.full.at[self.layer, pl.ds(pl.multiple_of(number * self.rows + i * size, 16), size), :]

    def load(self):
        pairs = ((self.at(self.me, self.w_from), self.at(self.me)), (self.m_from, self.m), (self.v_from, self.v))
        return [pltpu.make_async_copy(src, dst, self.loads.at[self.k, i]) for i, (src, dst) in enumerate(pairs)]

    def update(self, factor):
        w_ref = self.at(self.me)
        for copy in self.load():
            copy.wait()

        def chunk(rows, _):
            w, m, v = adamw(w_ref[rows, :].astype(F32), self.m[rows, :], self.v[rows, :], self.g[rows, :].astype(F32) * factor)
            w_ref[rows, :], self.m[rows, :], self.v[rows, :] = w, m, v

        each_row(self.rows, chunk)

    def copy(self, ref, number, to):
        return send(ref, ref, self.sems, (self.k, number), to)

    def own(self, i):
        return self.copy(self.at(self.me), i, (self.right, self.left, self.sibling)[i])

    def came(self, i):
        return self.copy(self.at((self.left, self.right, self.sibling)[i]), i, self.sibling)

    def on(self, i):
        return self.copy(self.half((self.left, self.right)[i], i), 3 + i, (self.right, self.left)[i])

    def opposite(self, i):
        return self.copy(self.half(self.place.block(2), i), 3 + i, self.sibling)

    def across(self, i):
        return self.copy(self.at((self.left, self.right)[i]) if i < 2 else self.half(self.place.block(2), i - 2), 5 + i, self.sibling)

    def came_across(self, i):
        of = self.place.sibling_block
        return self.copy(self.at(of((3, 1)[i])) if i < 2 else self.half(of(2), i - 2), 5 + i, self.sibling)

    def start(self):
        for i in range(3):
            self.own(i).start()

    def relay(self):
        for i in (0, 1):
            self.came(i).wait_recv()
            self.on(i).start()
            self.across(i).start()

    def finish(self):
        for i in (0, 1):
            self.opposite(i).wait_recv()
            self.across(2 + i).start()

    def end(self):
        self.came(2).wait_recv()
        for i in range(3):
            self.own(i).wait_send()
        for i in (0, 1):
            self.on(i).wait_send()
        for i in range(4):
            self.across(i).wait_send()
            self.came_across(i).wait_recv()


def update_kernel(devices, wide, tall, total, *refs):
    ws, ms, vs, full, new_m, new_v, (loads, sends, recvs) = (refs[i : i + 3] for i in range(0, 21, 3))
    place = Place(devices)
    work = []
    for k in range(6):
        a, layer = (k + 2) % 3, 1 - k // 3
        g = tall.at[1 - layer] if a == 2 else wide.at[2 * (1 - layer) + a]
        work.append(Piece(k, place, layer, full[a], new_m[a], new_v[a], ws[a], ms[a], vs[a], g, loads, (sends, recvs)))
    for piece in work[:2]:
        for copy in piece.load():
            copy.start()
    place.barrier([place.block(1), place.block(3), place.sibling_block(0)])
    count = sum(w.shape[0] * w.shape[1] * w.shape[2] for w in ws)
    factor = jnp.minimum(1.0, 0.5 * lax.rsqrt(jnp.sum(total[...], keepdims=True) / count + 1e-30))
    for k, piece in enumerate(work):
        piece.update(factor)
        piece.start()
        for copy in work[k + 2].load() if k + 2 < len(work) else []:
            copy.start()
    for k, piece in enumerate(work):
        piece.relay()
        if k:
            work[k - 1].finish()
    work[-1].finish()
    for piece in work:
        piece.end()


def store_kernel(*refs):
    count = len(refs) // 2
    copies = [pltpu.make_async_copy(refs[i], refs[count + i], refs[-1].at[i]) for i in range(count)]
    for copy in copies:
        copy.start()
    for copy in copies:
        copy.wait()


def updated(wide, tall, total, ws, ms, vs, devices):
    out = [*ws, *ms, *vs]
    anywhere, vmem = pl.BlockSpec(memory_space=pl.ANY), pl.BlockSpec(memory_space=pltpu.VMEM)
    new = pl.pallas_call(
        functools.partial(update_kernel, devices),
        in_specs=[vmem] * 3 + [anywhere] * 9,
        out_specs=[vmem] * 9,
        out_shape=[pltpu.VMEM(o.shape, o.dtype) for o in out],
        scratch_shapes=[pltpu.SemaphoreType.DMA((6, 3)), pltpu.SemaphoreType.DMA((6, 9)), pltpu.SemaphoreType.DMA((6, 9))],
        compiler_params=pltpu.CompilerParams(vmem_limit_bytes=4 * 1024 * 1024, collective_id=1, has_side_effects=True),
        name="update",
    )(*[pltpu.with_memory_space_constraint(g, pltpu.VMEM) for g in (wide, tall, total)], *[pltpu.with_memory_space_constraint(o, pltpu.HBM) for o in out])
    return pl.pallas_call(
        store_kernel,
        in_specs=[vmem] * 9,
        out_specs=[anywhere] * 9,
        out_shape=[jax.ShapeDtypeStruct(o.shape, o.dtype) for o in out],
        scratch_shapes=[pltpu.SemaphoreType.DMA((9,))],
        compiler_params=pltpu.CompilerParams(vmem_limit_bytes=1024 * 1024),
        name="store",
    )(*[pltpu.with_memory_space_constraint(n, pltpu.VMEM) for n in new])


def solution(mesh):
    devices = mesh.shape["dp"]

    def body(x, dy, wg, wu, wd, *moments):
        b, at = row_local(x[0], dy[0], wg, wu, wd)
        wide, tall, total = summed_gradients(at, b, devices)
        return tuple(updated(wide, tall, total, (wg, wu, wd), moments[:3], moments[3:], devices))

    data, whole, rows = P(("rep", "dp")), P(), P(None, "dp")
    return jax.shard_map(
        body,
        mesh=mesh,
        in_specs=(data, data, whole, whole, whole, *[rows] * 6),
        out_specs=(*[P("rep")] * 3, *[P("rep", "dp")] * 6),
        check_vma=False,
    )
```

```python
import functools

import jax
import jax.numpy as jnp
from jax import lax
from jax.experimental import pallas as pl
from jax.experimental.pallas import tpu as pltpu
from jax.sharding import PartitionSpec as P

F32, BF16 = jnp.float32, jnp.bfloat16
VMEM_LIMIT = 63 * 1024 * 1024
NT = (((1,), (1,)), ((), ()))
GRADS_LIMIT = 61850 * 1024
TILE, FEW = 512, 256
ROWS = 256


def dot(a, b, dims=(((1,), (0,)), ((), ()))):
    return lax.dot_general(a, b, dims, preferred_element_type=F32)


def scale_of(wide):
    return lax.rsqrt(jnp.mean(wide * wide, -1, keepdims=True) + 1e-6)


def normed(h):
    wide = h.astype(F32)
    return (wide * scale_of(wide)).astype(BF16)


def chunks(total, size):
    return [slice(at, min(at + size, total)) for at in range(0, total, size)]


def gated(gate, up, dact):
    s = jax.nn.sigmoid(gate)
    silu = gate * s
    return (dact * up * (s + silu * (1 - s))).astype(BF16), (dact * silu).astype(BF16)


def rows_kernel(x, dy, wg, wu, wd, b, gu, at, dh, held_wide, held_down, arrived):
    order = [(wg.at[0], held_wide.at[0]), (wu.at[0], held_wide.at[1]), (wd.at[0], held_down.at[0])]
    order += [(wg.at[1], held_wide.at[2]), (wu.at[1], held_wide.at[3]), (wd.at[1], held_down.at[1])]
    copies = [pltpu.make_async_copy(src, dst, arrived.at[n]) for n, (src, dst) in enumerate(order)]
    wg0, wu0, wd0, wg1, wu1, wd1 = (dst for _, dst in order)
    cols = chunks(wg.shape[2], 512)

    def tile(need):
        a = normed(x[...])
        at[3] = a.T
        d = dy[...]
        at[0] = d.T
        need(0, 1)
        for c in cols:
            gate, up = dot(a, wg0[:, c]), dot(a, wu0[:, c])
            gu[0, :, c], gu[1, :, c] = gate, up
            b[3, :, c] = (jax.nn.silu(gate) * up).astype(BF16)
        need(2)
        h = x[...] + dot(b[3], wd0[...]).astype(BF16)
        a = normed(h)
        at[1] = a.T
        need(3, 4, 5)
        for c in cols:
            gate, up = dot(a, wg1[:, c]), dot(a, wu1[:, c])
            dact = dot(d, wd1[c, :], NT).astype(BF16).astype(F32)
            b[2, :, c] = (jax.nn.silu(gate) * up).astype(BF16)
            b[0, :, c], b[1, :, c] = gated(gate, up, dact)
        da = (dot(wg1[...], b[0], NT).astype(BF16) + dot(wu1[...], b[1], NT).astype(BF16)).T
        da, wide = da.astype(F32), h.astype(F32)
        scale = scale_of(wide)
        inner = jnp.mean(da * wide, -1, keepdims=True)
        d = d + (da * scale - wide * (scale * scale * scale * inner)).astype(BF16)
        dh[...] = d
        at[2] = d.T

    first = pl.program_id(0) == 0

    @pl.when(first)
    def _():
        for copy in copies:
            copy.start()

        def need(*which):
            for n in which:
                copies[n].wait()

        tile(need)

    @pl.when(jnp.logical_not(first))
    def _():
        tile(lambda *which: None)


def row_local(x, dy, wg, wu, wd):
    t, d = x.shape
    f = wg.shape[2]
    rows, anywhere = pl.BlockSpec((ROWS, d), lambda i: (i, 0)), pl.BlockSpec(memory_space=pl.ANY)
    return pl.pallas_call(
        rows_kernel,
        grid=(t // ROWS,),
        in_specs=[rows, rows] + [anywhere] * 3,
        out_specs=[
            pl.BlockSpec((4, ROWS, f), lambda i: (0, i, 0)), pl.BlockSpec((2, ROWS, f), lambda i: (0, i, 0)),
            pl.BlockSpec((4, d, ROWS), lambda i: (0, 0, i)), rows,
        ],
        out_shape=[
            jax.ShapeDtypeStruct((4, t, f), BF16), jax.ShapeDtypeStruct((2, t, f), F32), jax.ShapeDtypeStruct((4, d, t), BF16),
            jax.ShapeDtypeStruct((t, d), BF16),
        ],
        scratch_shapes=[
            pltpu.VMEM((4, d, f), BF16), pltpu.VMEM((2, f, d), BF16),
            pltpu.SemaphoreType.DMA((6,)),
        ],
        compiler_params=pltpu.CompilerParams(vmem_limit_bytes=VMEM_LIMIT),
        cost_estimate=pl.CostEstimate(flops=16 * t * d * f, bytes_accessed=150 * 2**20, transcendentals=0),
        name="rows",
    )(x, dy, wg, wu, wd)


class Place:
    def __init__(self, devices):
        assert devices == 8
        self.devices = devices
        self.me = lax.axis_index("dp")
        self.chip, self.core = self.me // 2, self.me % 2

    def block(self, step):
        return (self.chip + step) % 4 * 2 + self.core

    def sibling_block(self, step):
        return (self.chip + step) % 4 * 2 + 1 - self.core

    def barrier(self, peers):
        semaphore = pltpu.get_barrier_semaphore()
        for peer in peers:
            pl.semaphore_signal(semaphore, inc=1, device_id={"dp": peer}, device_id_type=pl.DeviceIdType.MESH)
        pl.semaphore_wait(semaphore, len(peers))


def send(src, dst, sems, at, to):
    return pltpu.make_async_remote_copy(
        src_ref=src, dst_ref=dst, send_sem=sems[0].at[at], recv_sem=sems[1].at[at], device_id={"dp": to}, device_id_type=pl.DeviceIdType.MESH
    )


def each_row(count, body, size=16):
    lax.fori_loop(0, count // size, lambda i, c: body(pl.ds(pl.multiple_of(i * size, size), size), c) or c, 0)


def grads_kernel(
    devices, at, b, wd, gu_from, dh_from, out_wide, out_tall, out_total,
    wide, tall, sib_wide, sib_tall, transit_wide, transit_tall, end_wide, end_tall, gu, dh, both, part, totals, loaded, sends, recvs,
):
    step = pl.program_id(0)
    which, tile = step // 5, step % 5
    place = Place(devices)
    me = place.me
    peers = [(me + j) % devices for j in range(1, devices)]
    sibling = place.sibling_block(0)
    sems = (sends, recvs)
    low, high = wide.shape[1] // devices, tall.shape[1] // devices
    width = wide.shape[2]

    @pl.when(step == 0)
    def _():
        part[...] = jnp.zeros_like(part)
        place.barrier(peers)

    class Sum:
        def __init__(self, number, k, ready, start=0, size=None):
            self.number, n = number, k // 3
            self.is_tall, self.ready = k in (2, 3), ready
            self.end_by = (20, 20, 32, 32, 33, 33)[k]
            size = size or width
            if self.is_tall:
                self.rows, self.cols, self.mine, self.sib = high, slice(None), tall.at[n], sib_tall.at[n]
                self.transit, self.end, self.out = [transit_tall.at[n, i] for i in (0, 1)], [end_tall.at[n, i] for i in (0, 1)], out_tall.at[n]
                self.halves = [(pl.ds(i * high // 2, high // 2), slice(None)) for i in (0, 1)]
            else:
                slot = k % 4
                at = 2 * n + slot
                self.rows, self.cols, self.mine, self.sib = low, pl.ds(start, size), wide.at[slot], sib_wide.at[slot]
                c = size // 2
                self.transit = [transit_wide.at[slot, i, :, pl.ds(start // 2, c)] for i in (0, 1)]
                self.end, self.out = [end_wide.at[slot, i] for i in (0, 1)], out_wide.at[at]
                self.halves = [(slice(None), pl.ds(start + i * c, c)) for i in (0, 1)]

        def block(self, number):
            return self.mine.at[pl.ds(pl.multiple_of(number * self.rows, 16), self.rows), self.cols]

        def half(self, number, i):
            start, size = (i * self.rows // 2, self.rows // 2) if self.is_tall else (0, self.rows)
            return self.mine.at[pl.ds(pl.multiple_of(number * self.rows + start, 16), size), self.halves[i][1]]

        def theirs(self, j):
            return self.sib.at[j, :, self.cols]

        def to_sibling(self, j):
            return send(self.block(place.sibling_block(j)), self.theirs(j), sems, (self.number, j), sibling)

        def in_transit(self, i):
            return send(self.half(place.block(2), i), self.transit[i], sems, (self.number, 4 + i), place.block(1 - 2 * i))

        def to_end(self, i, j):
            copy = (8 if i == j else 6) + i
            return send(self.half(place.block(1 - 2 * i), j), self.end[i].at[self.halves[j]], sems, (self.number, copy), place.block(1 - 2 * i))

        def start(self):
            for j in (2, 1, 3, 0):
                self.to_sibling(j).start()

        def add(self, mine, theirs):
            def add(rows, _):
                mine[rows, :] = (mine[rows, :].astype(F32) + theirs[rows, :].astype(F32)).astype(BF16)

            each_row(mine.shape[0], add)

        def first(self):
            for j in (2, 1, 3, 0):
                self.to_sibling(j).wait_recv()
                self.add(self.block(place.block(j)), self.theirs(j))
                if j == 2:
                    for i in (0, 1):
                        self.in_transit(i).start()
                if j in (1, 3):
                    self.to_end(j // 2, 1 - j // 2).start()

        def second(self):
            for i in (0, 1):
                self.in_transit(i).wait_recv()
                self.add(self.half(place.block(1 - 2 * i), i), self.transit[i])
                self.to_end(i, i).start()

        def last(self):
            for i in (0, 1):
                for j in (0, 1):
                    self.to_end(i, j).wait_recv()
            mine, out = self.block(me), self.out.at[:, self.cols]
            ends = [end.at[:, self.cols] for end in self.end]

            def add(rows, total):
                g = (mine[rows, :].astype(F32) + ends[0][rows, :].astype(F32) + ends[1][rows, :].astype(F32)).astype(BF16)
                out[rows, :] = g
                g = g.astype(F32)
                return total + g[:8] * g[:8] + g[8:] * g[8:]

            cols = mine.shape[1]
            square = lax.fori_loop(0, self.rows // 16, lambda i, c: add(pl.ds(pl.multiple_of(i * 16, 16), 16), c), jnp.zeros((8, cols), F32))
            for c in chunks(cols, 128):
                part[...] += square[:, c]
            for j in (2, 1, 3, 0):
                self.to_sibling(j).wait_send()
            for i in (0, 1):
                self.in_transit(i).wait_send()
                for j in (0, 1):
                    self.to_end(i, j).wait_send()

    parts = [(0, 1, 0, TILE), (0, 3, TILE, 2 * TILE), (0, 5, 3 * TILE, 2 * TILE), (1, 7, 0, 2 * TILE), (1, 10, 2 * TILE, 3 * TILE)]
    parts += [(2, 15), (3, 20)] + [(k, ready, at * FEW, size * FEW) for ready, at, size in ((24, 0, 4), (27, 4, 3), (30, 7, 3)) for k in (4, 5)]
    sums = [Sum(n, *of) for n, of in enumerate(parts)]
    moves = []
    for one in sums:
        moves += [(one.ready, 0, one.start), (one.ready + 1, 1, one.first), (one.ready + 3 - one.ready // 30, 2, one.second), (one.end_by, 3, one.last)]
    moves.sort(key=lambda move: move[:2])
    for due in range(30):
        now = [move for when, _, move in moves if when == due]
        if now:

            @pl.when(step == due)
            def _():
                for move in now:
                    move()

    def columns(number):
        cols = pl.ds(pl.multiple_of(number * FEW, FEW), FEW)
        return pltpu.make_async_copy(gu_from.at[:, :, cols], gu.at[number % 2], loaded.at[number % 2])

    rest = pltpu.make_async_copy(dh_from, dh, loaded.at[2])
    column = step - 20

    @pl.when(step == 1)
    def _():
        rest.start()

    @pl.when((step >= 19) & (step < 29))
    def _():
        columns(column + 1).start()

    @pl.when(step < 20)
    def _():
        @pl.when(which >= 2)
        def _():
            tall[which - 2, pl.ds(pl.multiple_of(tile * TILE, TILE), TILE), :] = dot(at[...], b[...]).astype(BF16).T

        @pl.when(which < 2)
        def _():
            wide[which, :, pl.ds(pl.multiple_of(tile * TILE, TILE), TILE)] = dot(at[...], b[...]).astype(BF16)

    @pl.when(step == 20)
    def _():
        rest.wait()

    @pl.when(step >= 20)
    def _():
        columns(column).wait()
        held = gu.at[column % 2]
        for r in chunks(dh.shape[0], 512):
            dact = dot(dh[r, :], wd[...], NT).astype(BF16).astype(F32)
            both[r, :FEW], both[r, FEW:] = gated(held[0, r, :], held[1, r, :], dact)
        cols = pl.ds(pl.multiple_of(column * FEW, FEW), FEW)
        g = dot(at[...], both[...]).astype(BF16)
        wide[0, :, cols], wide[1, :, cols] = g[:, :FEW], g[:, FEW:]

    @pl.when(step == 29)
    def _():
        for due, _, move in moves:
            if due >= 30:
                move()
        exchange = [send(part, totals.at[j], sems, (len(sums), j), peer) for j, peer in enumerate(peers)]
        for copy in exchange:
            copy.start()
        total = part[...]
        for copy in exchange:
            copy.wait_recv()
        for j in range(len(peers)):
            total += totals[j]
        out_total[...] = total
        for copy in exchange:
            copy.wait_send()


def summed_gradients(at, b, wd, gu, dh, devices):
    (_, d, t), f = at.shape, b.shape[2]
    low, high = d // devices, f // devices
    vmem = pltpu.VMEM
    whole, anywhere = pl.BlockSpec(memory_space=vmem), pl.BlockSpec(memory_space=pl.ANY)
    operand = lambda i: (1 - i // 10 + 2 * (i // 15) + 2 * (i // 20), 0, 0)
    tile = lambda i: (jnp.minimum(i, 19) // 5, 0, jnp.minimum(i, 19) % 5)
    return pl.pallas_call(
        functools.partial(grads_kernel, devices),
        grid=(30,),
        in_specs=[
            pl.BlockSpec((pl.squeezed, d, t), operand), pl.BlockSpec((pl.squeezed, t, TILE), tile),
            pl.BlockSpec((pl.squeezed, FEW, d), lambda i: (0, jnp.maximum(i - 20, 0), 0)), anywhere, anywhere,
        ],
        out_specs=[whole] * 3,
        out_shape=[vmem((4, low, f), BF16), vmem((2, high, d), BF16), vmem((8, 128), F32)],
        scratch_shapes=[
            vmem((2, d, f), BF16), vmem((2, f, d), BF16), vmem((2, 4, low, f), BF16), vmem((2, 4, high, d), BF16),
            vmem((2, 2, low, f // 2), BF16), vmem((2, 2, high // 2, d), BF16), vmem((2, 2, low, f), BF16), vmem((2, 2, high, d), BF16),
            vmem((2, 2, t, FEW), F32), vmem((t, d), BF16), vmem((t, 2 * FEW), BF16),
            vmem((8, 128), F32), vmem((devices - 1, 8, 128), F32),
            pltpu.SemaphoreType.DMA((3,)), pltpu.SemaphoreType.DMA((14, 10)), pltpu.SemaphoreType.DMA((14, 10)),
        ],
        compiler_params=pltpu.CompilerParams(vmem_limit_bytes=GRADS_LIMIT, collective_id=0, has_side_effects=True),
        cost_estimate=pl.CostEstimate(flops=14 * t * d * f, bytes_accessed=120 * 2**20, transcendentals=0),
        name="grads",
    )(at, b, wd, *[pltpu.with_memory_space_constraint(one, pltpu.HBM) for one in (gu, dh)])


def adamw(w, m, v, g):
    m = 0.9 * m + 0.1 * g
    v = 0.95 * v + 0.05 * g * g
    step = m * lax.rsqrt(v + 1e-8) + 0.1 * w
    return (w - 0.02 * step).astype(BF16), m, v


class Piece:
    def __init__(self, k, place, layer, full, m, v, w_from, m_from, v_from, g, loads, sems):
        self.k, self.place, self.layer, self.full = k, place, layer, full
        self.m, self.v, self.g, self.sems, self.loads = m.at[layer], v.at[layer], g, sems, loads
        self.w_from, self.m_from, self.v_from = w_from, m_from.at[layer], v_from.at[layer]
        self.rows, self.cols = m.shape[1:]
        self.me, self.right, self.left, self.sibling = place.me, place.block(1), place.block(3), place.sibling_block(0)

    def at(self, number, of=None):
        return (self.full if of is None else of).at[self.layer, pl.ds(pl.multiple_of(number * self.rows, 16), self.rows), :]

    def half(self, number, i):
        if self.rows % 32:
            size = self.cols // 2
            return self.full.at[self.layer, pl.ds(pl.multiple_of(number * self.rows, 16), self.rows), pl.ds(i * size, size)]
        size = self.rows // 2
        return self.full.at[self.layer, pl.ds(pl.multiple_of(number * self.rows + i * size, 16), size), :]

    def load(self):
        pairs = ((self.at(self.me, self.w_from), self.at(self.me)), (self.m_from, self.m), (self.v_from, self.v))
        return [pltpu.make_async_copy(src, dst, self.loads.at[self.k, i]) for i, (src, dst) in enumerate(pairs)]

    def update(self, factor):
        w_ref = self.at(self.me)
        for copy in self.load():
            copy.wait()

        def chunk(rows, _):
            w, m, v = adamw(w_ref[rows, :].astype(F32), self.m[rows, :], self.v[rows, :], self.g[rows, :].astype(F32) * factor)
            w_ref[rows, :], self.m[rows, :], self.v[rows, :] = w, m, v

        each_row(self.rows, chunk)

    def copy(self, ref, number, to):
        return send(ref, ref, self.sems, (self.k, number), to)

    def own(self, i):
        return self.copy(self.at(self.me), i, (self.right, self.left, self.sibling)[i])

    def came(self, i):
        return self.copy(self.at((self.left, self.right, self.sibling)[i]), i, self.sibling)

    def on(self, i):
        return self.copy(self.half((self.left, self.right)[i], i), 3 + i, (self.right, self.left)[i])

    def opposite(self, i):
        return self.copy(self.half(self.place.block(2), i), 3 + i, self.sibling)

    def across(self, i):
        return self.copy(self.at((self.left, self.right)[i]) if i < 2 else self.half(self.place.block(2), i - 2), 5 + i, self.sibling)

    def came_across(self, i):
        of = self.place.sibling_block
        return self.copy(self.at(of((3, 1)[i])) if i < 2 else self.half(of(2), i - 2), 5 + i, self.sibling)

    def start(self):
        for i in range(3):
            self.own(i).start()

    def relay(self):
        for i in (0, 1):
            self.came(i).wait_recv()
            self.on(i).start()
            self.across(i).start()

    def finish(self):
        for i in (0, 1):
            self.opposite(i).wait_recv()
            self.across(2 + i).start()

    def end(self):
        self.came(2).wait_recv()
        for i in range(3):
            self.own(i).wait_send()
        for i in (0, 1):
            self.on(i).wait_send()
        for i in range(4):
            self.across(i).wait_send()
            self.came_across(i).wait_recv()


def update_kernel(devices, wide, tall, total, *refs):
    ws, ms, vs, full, new_m, new_v, (loads, sends, recvs) = (refs[i : i + 3] for i in range(0, 21, 3))
    place = Place(devices)
    work = []
    for k in range(6):
        a, layer = (k + 2) % 3, 1 - k // 3
        g = tall.at[1 - layer] if a == 2 else wide.at[2 * (1 - layer) + a]
        work.append(Piece(k, place, layer, full[a], new_m[a], new_v[a], ws[a], ms[a], vs[a], g, loads, (sends, recvs)))
    for piece in work[:2]:
        for copy in piece.load():
            copy.start()
    place.barrier([place.block(1), place.block(3), place.sibling_block(0)])
    count = sum(w.shape[0] * w.shape[1] * w.shape[2] for w in ws)
    factor = jnp.minimum(1.0, 0.5 * lax.rsqrt(jnp.sum(total[...], keepdims=True) / count + 1e-30))
    for k, piece in enumerate(work):
        piece.update(factor)
        piece.start()
        for copy in work[k + 2].load() if k + 2 < len(work) else []:
            copy.start()
    for k, piece in enumerate(work):
        piece.relay()
        if k:
            work[k - 1].finish()
    work[-1].finish()
    for piece in work:
        piece.end()


def store_kernel(*refs):
    count = len(refs) // 2
    copies = [pltpu.make_async_copy(refs[i], refs[count + i], refs[-1].at[i]) for i in range(count)]
    for copy in copies:
        copy.start()
    for copy in copies:
        copy.wait()


def updated(wide, tall, total, ws, ms, vs, devices):
    out = [*ws, *ms, *vs]
    anywhere, vmem = pl.BlockSpec(memory_space=pl.ANY), pl.BlockSpec(memory_space=pltpu.VMEM)
    new = pl.pallas_call(
        functools.partial(update_kernel, devices),
        in_specs=[vmem] * 3 + [anywhere] * 9,
        out_specs=[vmem] * 9,
        out_shape=[pltpu.VMEM(o.shape, o.dtype) for o in out],
        scratch_shapes=[pltpu.SemaphoreType.DMA((6, 3)), pltpu.SemaphoreType.DMA((6, 9)), pltpu.SemaphoreType.DMA((6, 9))],
        compiler_params=pltpu.CompilerParams(vmem_limit_bytes=4 * 1024 * 1024, collective_id=1, has_side_effects=True),
        name="update",
    )(*[pltpu.with_memory_space_constraint(g, pltpu.VMEM) for g in (wide, tall, total)], *[pltpu.with_memory_space_constraint(o, pltpu.HBM) for o in out])
    return pl.pallas_call(
        store_kernel,
        in_specs=[vmem] * 9,
        out_specs=[anywhere] * 9,
        out_shape=[jax.ShapeDtypeStruct(o.shape, o.dtype) for o in out],
        scratch_shapes=[pltpu.SemaphoreType.DMA((9,))],
        compiler_params=pltpu.CompilerParams(vmem_limit_bytes=1024 * 1024),
        name="store",
    )(*[pltpu.with_memory_space_constraint(n, pltpu.VMEM) for n in new])


def solution(mesh):
    devices = mesh.shape["dp"]

    def body(x, dy, wg, wu, wd, *moments):
        b, gu, at, dh = row_local(x[0], dy[0], wg, wu, wd)
        wide, tall, total = summed_gradients(at, b, wd, gu, dh, devices)
        return tuple(updated(wide, tall, total, (wg, wu, wd), moments[:3], moments[3:], devices))

    data, whole, rows = P(("rep", "dp")), P(), P(None, "dp")
    return jax.shard_map(
        body,
        mesh=mesh,
        in_specs=(data, data, whole, whole, whole, *[rows] * 6),
        out_specs=(*[P("rep")] * 3, *[P("rep", "dp")] * 6),
        check_vma=False,
    )
```

```python
import functools

import jax
import jax.numpy as jnp
from jax import lax
from jax.experimental import pallas as pl
from jax.experimental.pallas import tpu as pltpu
from jax.sharding import PartitionSpec as P

F32, BF16 = jnp.float32, jnp.bfloat16
VMEM_LIMIT = 63 * 1024 * 1024
NT = (((1,), (1,)), ((), ()))
GRADS_LIMIT = 61850 * 1024
TILE, FEW = 512, 256
ROWS = 256


def dot(a, b, dims=(((1,), (0,)), ((), ()))):
    return lax.dot_general(a, b, dims, preferred_element_type=F32)


def scale_of(wide):
    return lax.rsqrt(jnp.mean(wide * wide, -1, keepdims=True) + 1e-6)


def normed(h):
    wide = h.astype(F32)
    return (wide * scale_of(wide)).astype(BF16)


def chunks(total, size):
    return [slice(at, min(at + size, total)) for at in range(0, total, size)]


def gated(gate, up, dact):
    s = jax.nn.sigmoid(gate)
    silu = gate * s
    return (dact * up * (s + silu * (1 - s))).astype(BF16), (dact * silu).astype(BF16)


def rows_kernel(x, dy, wg, wu, wd, b, gu, at, dh, held_wide, held_down, arrived):
    order = [(wg.at[0], held_wide.at[0]), (wu.at[0], held_wide.at[1]), (wd.at[0], held_down.at[0])]
    order += [(wg.at[1], held_wide.at[2]), (wu.at[1], held_wide.at[3]), (wd.at[1], held_down.at[1])]
    copies = [pltpu.make_async_copy(src, dst, arrived.at[n]) for n, (src, dst) in enumerate(order)]
    wg0, wu0, wd0, wg1, wu1, wd1 = (dst for _, dst in order)
    cols = chunks(wg.shape[2], 512)

    def tile(need):
        a = normed(x[...])
        at[3] = a.T
        d = dy[...]
        at[0] = d.T
        need(0, 1)
        for c in cols:
            gate, up = dot(a, wg0[:, c]), dot(a, wu0[:, c])
            gu[0, :, c], gu[1, :, c] = gate, up
            b[3, :, c] = (jax.nn.silu(gate) * up).astype(BF16)
        need(2)
        h = x[...] + dot(b[3], wd0[...]).astype(BF16)
        a = normed(h)
        at[1] = a.T
        need(3, 4, 5)
        for c in cols:
            gate, up = dot(a, wg1[:, c]), dot(a, wu1[:, c])
            dact = dot(d, wd1[c, :], NT).astype(BF16).astype(F32)
            b[2, :, c] = (jax.nn.silu(gate) * up).astype(BF16)
            b[0, :, c], b[1, :, c] = gated(gate, up, dact)
        da = (dot(wg1[...], b[0], NT).astype(BF16) + dot(wu1[...], b[1], NT).astype(BF16)).T
        da, wide = da.astype(F32), h.astype(F32)
        scale = scale_of(wide)
        inner = jnp.mean(da * wide, -1, keepdims=True)
        d = d + (da * scale - wide * (scale * scale * scale * inner)).astype(BF16)
        dh[...] = d
        at[2] = d.T

    first = pl.program_id(0) == 0

    @pl.when(first)
    def _():
        for copy in copies:
            copy.start()

        def need(*which):
            for n in which:
                copies[n].wait()

        tile(need)

    @pl.when(jnp.logical_not(first))
    def _():
        tile(lambda *which: None)


def row_local(x, dy, wg, wu, wd):
    t, d = x.shape
    f = wg.shape[2]
    rows, anywhere = pl.BlockSpec((ROWS, d), lambda i: (i, 0)), pl.BlockSpec(memory_space=pl.ANY)
    return pl.pallas_call(
        rows_kernel,
        grid=(t // ROWS,),
        in_specs=[rows, rows] + [anywhere] * 3,
        out_specs=[
            pl.BlockSpec((4, ROWS, f), lambda i: (0, i, 0)), pl.BlockSpec((2, ROWS, f), lambda i: (0, i, 0)),
            pl.BlockSpec((4, d, ROWS), lambda i: (0, 0, i)), rows,
        ],
        out_shape=[
            jax.ShapeDtypeStruct((4, t, f), BF16), jax.ShapeDtypeStruct((2, t, f), F32), jax.ShapeDtypeStruct((4, d, t), BF16),
            jax.ShapeDtypeStruct((t, d), BF16),
        ],
        scratch_shapes=[
            pltpu.VMEM((4, d, f), BF16), pltpu.VMEM((2, f, d), BF16),
            pltpu.SemaphoreType.DMA((6,)),
        ],
        compiler_params=pltpu.CompilerParams(vmem_limit_bytes=VMEM_LIMIT),
        cost_estimate=pl.CostEstimate(flops=16 * t * d * f, bytes_accessed=150 * 2**20, transcendentals=0),
        name="rows",
    )(x, dy, wg, wu, wd)


class Place:
    def __init__(self, devices):
        assert devices == 8
        self.devices = devices
        self.me = lax.axis_index("dp")
        self.chip, self.core = self.me // 2, self.me % 2

    def block(self, step):
        return (self.chip + step) % 4 * 2 + self.core

    def sibling_block(self, step):
        return (self.chip + step) % 4 * 2 + 1 - self.core

    def barrier(self, peers):
        semaphore = pltpu.get_barrier_semaphore()
        for peer in peers:
            pl.semaphore_signal(semaphore, inc=1, device_id={"dp": peer}, device_id_type=pl.DeviceIdType.MESH)
        pl.semaphore_wait(semaphore, len(peers))


def send(src, dst, sems, at, to):
    return pltpu.make_async_remote_copy(
        src_ref=src, dst_ref=dst, send_sem=sems[0].at[at], recv_sem=sems[1].at[at], device_id={"dp": to}, device_id_type=pl.DeviceIdType.MESH
    )


def each_row(count, body, size=16):
    lax.fori_loop(0, count // size, lambda i, c: body(pl.ds(pl.multiple_of(i * size, size), size), c) or c, 0)


def grads_kernel(
    devices, at, b, wd, gu_from, dh_from, out_wide, out_tall, out_total,
    wide, tall, sib_wide, sib_tall, transit_wide, transit_tall, end_wide, end_tall, gu, dh, both, part, totals, loaded, sends, recvs,
):
    step = pl.program_id(0)
    which, tile = step // 5, step % 5
    place = Place(devices)
    me = place.me
    peers = [(me + j) % devices for j in range(1, devices)]
    sibling = place.sibling_block(0)
    sems = (sends, recvs)
    low, high = wide.shape[1] // devices, tall.shape[1] // devices
    width = wide.shape[2]

    @pl.when(step == 0)
    def _():
        part[...] = jnp.zeros_like(part)
        place.barrier(peers)

    class Sum:
        def __init__(self, number, k, ready, start=0, size=None):
            self.number, n = number, k // 3
            self.is_tall, self.ready = k in (2, 3), ready
            self.patience = 2 if ready == 30 else 4 if 1 < ready < 20 else 3
            self.end_by = (20, 20, 32, 32, 33, 33)[k]
            size = size or width
            if self.is_tall:
                self.rows, self.cols, self.mine, self.sib = high, slice(None), tall.at[n], sib_tall.at[n]
                self.transit, self.end, self.out = [transit_tall.at[n, i] for i in (0, 1)], [end_tall.at[n, i] for i in (0, 1)], out_tall.at[n]
                self.halves = [(pl.ds(i * high // 2, high // 2), slice(None)) for i in (0, 1)]
            else:
                slot = k % 4
                at = 2 * n + slot
                self.rows, self.cols, self.mine, self.sib = low, pl.ds(start, size), wide.at[slot], sib_wide.at[slot]
                c = size // 2
                self.transit = [transit_wide.at[slot, i, :, pl.ds(start // 2, c)] for i in (0, 1)]
                self.end, self.out = [end_wide.at[slot, i] for i in (0, 1)], out_wide.at[at]
                self.halves = [(slice(None), pl.ds(start + i * c, c)) for i in (0, 1)]

        def block(self, number):
            return self.mine.at[pl.ds(pl.multiple_of(number * self.rows, 16), self.rows), self.cols]

        def half(self, number, i):
            start, size = (i * self.rows // 2, self.rows // 2) if self.is_tall else (0, self.rows)
            return self.mine.at[pl.ds(pl.multiple_of(number * self.rows + start, 16), size), self.halves[i][1]]

        def theirs(self, j):
            return self.sib.at[j, :, self.cols]

        def to_sibling(self, j):
            return send(self.block(place.sibling_block(j)), self.theirs(j), sems, (self.number, j), sibling)

        def in_transit(self, i):
            return send(self.half(place.block(2), i), self.transit[i], sems, (self.number, 4 + i), place.block(1 - 2 * i))

        def to_end(self, i, j):
            copy = (8 if i == j else 6) + i
            return send(self.half(place.block(1 - 2 * i), j), self.end[i].at[self.halves[j]], sems, (self.number, copy), place.block(1 - 2 * i))

        def start(self):
            for j in (2, 1, 3, 0):
                self.to_sibling(j).start()

        def add(self, mine, theirs):
            def add(rows, _):
                mine[rows, :] = (mine[rows, :].astype(F32) + theirs[rows, :].astype(F32)).astype(BF16)

            each_row(mine.shape[0], add)

        def first(self):
            for j in (2, 1, 3, 0):
                self.to_sibling(j).wait_recv()
                self.add(self.block(place.block(j)), self.theirs(j))
                if j == 2:
                    for i in (0, 1):
                        self.in_transit(i).start()
                if j in (1, 3):
                    self.to_end(j // 2, 1 - j // 2).start()

        def second(self):
            for i in (0, 1):
                self.in_transit(i).wait_recv()
                self.add(self.half(place.block(1 - 2 * i), i), self.transit[i])
                self.to_end(i, i).start()

        def last(self):
            for i in (0, 1):
                for j in (0, 1):
                    self.to_end(i, j).wait_recv()
            mine, out = self.block(me), self.out.at[:, self.cols]
            ends = [end.at[:, self.cols] for end in self.end]

            def add(rows, total):
                g = (mine[rows, :].astype(F32) + ends[0][rows, :].astype(F32) + ends[1][rows, :].astype(F32)).astype(BF16)
                out[rows, :] = g
                g = g.astype(F32)
                return total + g[:8] * g[:8] + g[8:] * g[8:]

            cols = mine.shape[1]
            square = lax.fori_loop(0, self.rows // 16, lambda i, c: add(pl.ds(pl.multiple_of(i * 16, 16), 16), c), jnp.zeros((8, cols), F32))
            for c in chunks(cols, 128):
                part[...] += square[:, c]
            for j in (2, 1, 3, 0):
                self.to_sibling(j).wait_send()
            for i in (0, 1):
                self.in_transit(i).wait_send()
                for j in (0, 1):
                    self.to_end(i, j).wait_send()

    parts = [(0, 1, 0, TILE), (0, 3, TILE, 2 * TILE), (0, 5, 3 * TILE, 2 * TILE), (1, 7, 0, 2 * TILE), (1, 10, 2 * TILE, 3 * TILE)]
    parts += [(2, 15), (3, 20)] + [(k, ready, at * FEW, size * FEW) for ready, at, size in ((24, 0, 4), (27, 4, 3), (30, 7, 3)) for k in (4, 5)]
    sums = [Sum(n, *of) for n, of in enumerate(parts)]
    moves = []
    for one in sums:
        moves += [(one.ready, 0, one.start), (one.ready + 1, 1, one.first), (one.ready + one.patience, 2, one.second), (one.end_by, 3, one.last)]
    moves.sort(key=lambda move: move[:2])
    for due in range(30):
        now = [move for when, _, move in moves if when == due]
        if now:

            @pl.when(step == due)
            def _():
                for move in now:
                    move()

    def columns(number):
        cols = pl.ds(pl.multiple_of(number * FEW, FEW), FEW)
        return pltpu.make_async_copy(gu_from.at[:, :, cols], gu.at[number % 2], loaded.at[number % 2])

    rest = pltpu.make_async_copy(dh_from, dh, loaded.at[2])
    column = step - 20

    @pl.when(step == 1)
    def _():
        rest.start()

    @pl.when((step >= 19) & (step < 29))
    def _():
        columns(column + 1).start()

    @pl.when(step < 20)
    def _():
        @pl.when(which >= 2)
        def _():
            tall[which - 2, pl.ds(pl.multiple_of(tile * TILE, TILE), TILE), :] = dot(at[...], b[...]).astype(BF16).T

        @pl.when(which < 2)
        def _():
            wide[which, :, pl.ds(pl.multiple_of(tile * TILE, TILE), TILE)] = dot(at[...], b[...]).astype(BF16)

    @pl.when(step == 20)
    def _():
        rest.wait()

    @pl.when(step >= 20)
    def _():
        columns(column).wait()
        held = gu.at[column % 2]
        for r in chunks(dh.shape[0], 512):
            dact = dot(dh[r, :], wd[...], NT).astype(BF16).astype(F32)
            both[r, :FEW], both[r, FEW:] = gated(held[0, r, :], held[1, r, :], dact)
        cols = pl.ds(pl.multiple_of(column * FEW, FEW), FEW)
        g = dot(at[...], both[...]).astype(BF16)
        wide[0, :, cols], wide[1, :, cols] = g[:, :FEW], g[:, FEW:]

    @pl.when(step == 29)
    def _():
        for due, _, move in moves:
            if due >= 30:
                move()
        exchange = [send(part, totals.at[j], sems, (len(sums), j), peer) for j, peer in enumerate(peers)]
        for copy in exchange:
            copy.start()
        total = part[...]
        for copy in exchange:
            copy.wait_recv()
        for j in range(len(peers)):
            total += totals[j]
        out_total[...] = total
        for copy in exchange:
            copy.wait_send()


def summed_gradients(at, b, wd, gu, dh, devices):
    (_, d, t), f = at.shape, b.shape[2]
    low, high = d // devices, f // devices
    vmem = pltpu.VMEM
    whole, anywhere = pl.BlockSpec(memory_space=vmem), pl.BlockSpec(memory_space=pl.ANY)
    operand = lambda i: (1 - i // 10 + 2 * (i // 15) + 2 * (i // 20), 0, 0)
    tile = lambda i: (jnp.minimum(i, 19) // 5, 0, jnp.minimum(i, 19) % 5)
    return pl.pallas_call(
        functools.partial(grads_kernel, devices),
        grid=(30,),
        in_specs=[
            pl.BlockSpec((pl.squeezed, d, t), operand), pl.BlockSpec((pl.squeezed, t, TILE), tile),
            pl.BlockSpec((pl.squeezed, FEW, d), lambda i: (0, jnp.maximum(i - 20, 0), 0)), anywhere, anywhere,
        ],
        out_specs=[whole] * 3,
        out_shape=[vmem((4, low, f), BF16), vmem((2, high, d), BF16), vmem((8, 128), F32)],
        scratch_shapes=[
            vmem((2, d, f), BF16), vmem((2, f, d), BF16), vmem((2, 4, low, f), BF16), vmem((2, 4, high, d), BF16),
            vmem((2, 2, low, f // 2), BF16), vmem((2, 2, high // 2, d), BF16), vmem((2, 2, low, f), BF16), vmem((2, 2, high, d), BF16),
            vmem((2, 2, t, FEW), F32), vmem((t, d), BF16), vmem((t, 2 * FEW), BF16),
            vmem((8, 128), F32), vmem((devices - 1, 8, 128), F32),
            pltpu.SemaphoreType.DMA((3,)), pltpu.SemaphoreType.DMA((14, 10)), pltpu.SemaphoreType.DMA((14, 10)),
        ],
        compiler_params=pltpu.CompilerParams(vmem_limit_bytes=GRADS_LIMIT, collective_id=0, has_side_effects=True),
        cost_estimate=pl.CostEstimate(flops=14 * t * d * f, bytes_accessed=120 * 2**20, transcendentals=0),
        name="grads",
    )(at, b, wd, *[pltpu.with_memory_space_constraint(one, pltpu.HBM) for one in (gu, dh)])


def adamw(w, m, v, g):
    m = 0.9 * m + 0.1 * g
    v = 0.95 * v + 0.05 * g * g
    step = m * lax.rsqrt(v + 1e-8) + 0.1 * w
    return (w - 0.02 * step).astype(BF16), m, v


class Piece:
    def __init__(self, k, place, layer, full, m, v, w_from, m_from, v_from, g, loads, sems):
        self.k, self.place, self.layer, self.full = k, place, layer, full
        self.m, self.v, self.g, self.sems, self.loads = m.at[layer], v.at[layer], g, sems, loads
        self.w_from, self.m_from, self.v_from = w_from, m_from.at[layer], v_from.at[layer]
        self.rows, self.cols = m.shape[1:]
        self.me, self.right, self.left, self.sibling = place.me, place.block(1), place.block(3), place.sibling_block(0)

    def at(self, number, of=None):
        return (self.full if of is None else of).at[self.layer, pl.ds(pl.multiple_of(number * self.rows, 16), self.rows), :]

    def half(self, number, i):
        if self.rows % 32:
            size = self.cols // 2
            return self.full.at[self.layer, pl.ds(pl.multiple_of(number * self.rows, 16), self.rows), pl.ds(i * size, size)]
        size = self.rows // 2
        return self.full.at[self.layer, pl.ds(pl.multiple_of(number * self.rows + i * size, 16), size), :]

    def load(self):
        pairs = ((self.at(self.me, self.w_from), self.at(self.me)), (self.m_from, self.m), (self.v_from, self.v))
        return [pltpu.make_async_copy(src, dst, self.loads.at[self.k, i]) for i, (src, dst) in enumerate(pairs)]

    def update(self, factor):
        w_ref = self.at(self.me)
        for copy in self.load():
            copy.wait()

        def chunk(rows, _):
            w, m, v = adamw(w_ref[rows, :].astype(F32), self.m[rows, :], self.v[rows, :], self.g[rows, :].astype(F32) * factor)
            w_ref[rows, :], self.m[rows, :], self.v[rows, :] = w, m, v

        each_row(self.rows, chunk)

    def copy(self, ref, number, to):
        return send(ref, ref, self.sems, (self.k, number), to)

    def own(self, i):
        return self.copy(self.at(self.me), i, (self.right, self.left, self.sibling)[i])

    def came(self, i):
        return self.copy(self.at((self.left, self.right, self.sibling)[i]), i, self.sibling)

    def on(self, i):
        return self.copy(self.half((self.left, self.right)[i], i), 3 + i, (self.right, self.left)[i])

    def opposite(self, i):
        return self.copy(self.half(self.place.block(2), i), 3 + i, self.sibling)

    def across(self, i):
        return self.copy(self.at((self.left, self.right)[i]) if i < 2 else self.half(self.place.block(2), i - 2), 5 + i, self.sibling)

    def came_across(self, i):
        of = self.place.sibling_block
        return self.copy(self.at(of((3, 1)[i])) if i < 2 else self.half(of(2), i - 2), 5 + i, self.sibling)

    def start(self):
        for i in range(3):
            self.own(i).start()

    def relay(self):
        for i in (0, 1):
            self.came(i).wait_recv()
            self.on(i).start()
            self.across(i).start()

    def finish(self):
        for i in (0, 1):
            self.opposite(i).wait_recv()
            self.across(2 + i).start()

    def end(self):
        self.came(2).wait_recv()
        for i in range(3):
            self.own(i).wait_send()
        for i in (0, 1):
            self.on(i).wait_send()
        for i in range(4):
            self.across(i).wait_send()
            self.came_across(i).wait_recv()


def update_kernel(devices, wide, tall, total, *refs):
    ws, ms, vs, full, new_m, new_v, (loads, sends, recvs) = (refs[i : i + 3] for i in range(0, 21, 3))
    place = Place(devices)
    work = []
    for k in range(6):
        a, layer = (k + 2) % 3, 1 - k // 3
        g = tall.at[1 - layer] if a == 2 else wide.at[2 * (1 - layer) + a]
        work.append(Piece(k, place, layer, full[a], new_m[a], new_v[a], ws[a], ms[a], vs[a], g, loads, (sends, recvs)))
    for piece in work[:2]:
        for copy in piece.load():
            copy.start()
    place.barrier([place.block(1), place.block(3), place.sibling_block(0)])
    count = sum(w.shape[0] * w.shape[1] * w.shape[2] for w in ws)
    factor = jnp.minimum(1.0, 0.5 * lax.rsqrt(jnp.sum(total[...], keepdims=True) / count + 1e-30))
    for k, piece in enumerate(work):
        piece.update(factor)
        piece.start()
        for copy in work[k + 2].load() if k + 2 < len(work) else []:
            copy.start()
    for k, piece in enumerate(work):
        piece.relay()
        if k:
            work[k - 1].finish()
    work[-1].finish()
    for piece in work:
        piece.end()


def store_kernel(*refs):
    count = len(refs) // 2
    copies = [pltpu.make_async_copy(refs[i], refs[count + i], refs[-1].at[i]) for i in range(count)]
    for copy in copies:
        copy.start()
    for copy in copies:
        copy.wait()


def updated(wide, tall, total, ws, ms, vs, devices):
    out = [*ws, *ms, *vs]
    anywhere, vmem = pl.BlockSpec(memory_space=pl.ANY), pl.BlockSpec(memory_space=pltpu.VMEM)
    new = pl.pallas_call(
        functools.partial(update_kernel, devices),
        in_specs=[vmem] * 3 + [anywhere] * 9,
        out_specs=[vmem] * 9,
        out_shape=[pltpu.VMEM(o.shape, o.dtype) for o in out],
        scratch_shapes=[pltpu.SemaphoreType.DMA((6, 3)), pltpu.SemaphoreType.DMA((6, 9)), pltpu.SemaphoreType.DMA((6, 9))],
        compiler_params=pltpu.CompilerParams(vmem_limit_bytes=4 * 1024 * 1024, collective_id=1, has_side_effects=True),
        name="update",
    )(*[pltpu.with_memory_space_constraint(g, pltpu.VMEM) for g in (wide, tall, total)], *[pltpu.with_memory_space_constraint(o, pltpu.HBM) for o in out])
    return pl.pallas_call(
        store_kernel,
        in_specs=[vmem] * 9,
        out_specs=[anywhere] * 9,
        out_shape=[jax.ShapeDtypeStruct(o.shape, o.dtype) for o in out],
        scratch_shapes=[pltpu.SemaphoreType.DMA((9,))],
        compiler_params=pltpu.CompilerParams(vmem_limit_bytes=1024 * 1024),
        name="store",
    )(*[pltpu.with_memory_space_constraint(n, pltpu.VMEM) for n in new])


def solution(mesh):
    devices = mesh.shape["dp"]

    def body(x, dy, wg, wu, wd, *moments):
        b, gu, at, dh = row_local(x[0], dy[0], wg, wu, wd)
        wide, tall, total = summed_gradients(at, b, wd, gu, dh, devices)
        return tuple(updated(wide, tall, total, (wg, wu, wd), moments[:3], moments[3:], devices))

    data, whole, rows = P(("rep", "dp")), P(), P(None, "dp")
    return jax.shard_map(
        body,
        mesh=mesh,
        in_specs=(data, data, whole, whole, whole, *[rows] * 6),
        out_specs=(*[P("rep")] * 3, *[P("rep", "dp")] * 6),
        check_vma=False,
    )
```
